128 devices in a mesh: row: 16 (over z, x), col: 8 (over y, core).
Axes of the slice: x: 4, y: 4, z: 4, core: 2. Of those that a mesh axis runs over, the one named last changes fastest.
Arguments:
- start_block: float32 [8, 131072], P(None, ('row', 'col')), may hold values from -6 to 6
- blocks: bfloat16 [16, 8, 128, 128, 128], P('row', 'col'), as said below
- block_rows: int32 [16, 8, 128], P(None, 'col'), may hold values from 0 to 63, as said below
- block_cols: int32 [16, 8, 128], P(None, 'col'), may hold values from 0 to 127, as said below
- counts: int32 [16, 8], replicated, may hold values from 1 to 128, as said below
Outputs:
- next_block: float32 [8, 131072], P(None, ('row', 'col'))
- tridiagonal: float32 [16, 16], replicated
The draws below stay inside these ranges and needn't reach their ends.
Inputs may be any that keep to these rules, and one draw needn't show every extreme that they name: `block_rows`: entries of each tile are local block rows below 64; within a tile the used slots name distinct blocks whose global row block is at or after the global column block; slots at or after counts are 0 and not part of H. `block_cols`: local block columns below 128, paired with block_rows; unused slots are 0. `counts`: some tile holds exactly 128 blocks in every draw. Blocks whose global row and column blocks agree are symmetric.
All inputs are finite; a program needn't handle non-finite values.
Results may differ from the reference program's by a relative error of at most 0.0048.
Values may be sent and summed in bfloat16 or wider, within the bound.
A program may use at most 64 MiB of HBM per device.

```python
import jax
import jax.numpy as jnp
from jax import lax

BS = 128
K = 8
ITERS = 2
M = 8
MAXB = 128
VP = 1024
NV = 131072
N_ROW = 16
N_COL = 8


def layout(key):
    base = jax.random.fold_in(key, 11)
    row_blocks = N_COL * M
    col_blocks = N_ROW * M
    pairs = row_blocks * col_blocks
    pair_ids = jnp.arange(pairs, dtype=jnp.int32)
    local_row = pair_ids // col_blocks
    local_col = pair_ids % col_blocks
    grid_row = jnp.arange(N_ROW, dtype=jnp.int32)[:, None, None]
    grid_col = jnp.arange(N_COL, dtype=jnp.int32)[None, :, None]
    global_row = grid_row * row_blocks + local_row[None, None, :]
    global_col = (local_col[None, None, :] // M * N_COL + grid_col) * M + local_col[None, None, :] % M
    allowed = global_row >= global_col
    candidates = jnp.sum(allowed.astype(jnp.int32), axis=-1)
    chosen_col = jax.random.randint(jax.random.fold_in(base, 1), (), 0, N_COL)
    anchor_count = candidates[N_ROW - 1, chosen_col]
    jitter = jax.random.randint(jax.random.fold_in(base, 2), (N_ROW, N_COL), 0, MAXB // 8 + 2)
    jitter = jnp.where(grid_row[:, :, 0] == N_ROW - 1, 0, jitter)
    target = candidates * MAXB // anchor_count - jitter
    counts = jnp.clip(target, 1, jnp.minimum(candidates, MAXB)).astype(jnp.int32)
    limit = 2 ** 30 // pairs
    scores = jax.random.randint(jax.random.fold_in(base, 3), (N_ROW, N_COL, pairs), 0, limit) * pairs + pair_ids[None, None, :]
    scores = jnp.where(allowed, scores, scores + 2 ** 30)
    order = jnp.argsort(scores, axis=-1, stable=True)[..., :MAXB]
    slot_ids = jnp.arange(MAXB, dtype=jnp.int32)
    used = slot_ids[None, None, :] < counts[..., None]
    rows = jnp.where(used, local_row[order], 0).astype(jnp.int32)
    cols = jnp.where(used, local_col[order], 0).astype(jnp.int32)
    return (rows, cols, counts)


def draw_block_rows(key, part):
    rows, cols, counts = layout(key)
    return rows


def draw_block_cols(key, part):
    rows, cols, counts = layout(key)
    return cols


def draw_counts(key, part):
    rows, cols, counts = layout(key)
    return counts


def draw_blocks(key, part):
    rows, cols, counts = layout(key)
    grid_row = jnp.arange(N_ROW, dtype=jnp.int32)[:, None, None]
    grid_col = jnp.arange(N_COL, dtype=jnp.int32)[None, :, None]
    global_row = grid_row * (N_COL * M) + rows
    global_col = (cols // M * N_COL + grid_col) * M + cols % M
    diagonal = global_row == global_col
    shape = (N_ROW, N_COL, MAXB, BS, BS)
    noise_key = jax.random.fold_in(key, 5)
    scale = (M / (MAXB * BS)) ** 0.5
    values = jax.random.normal(noise_key, shape, jnp.float32)
    values = values * scale
    mirrored = 0.5 * (values + jnp.swapaxes(values, -1, -2))
    return jnp.where(diagonal[..., None, None], mirrored, values).astype(jnp.bfloat16)


def steps_of(stream_key, extent, shards, smallest, top_value):
    loudness, own = 1.0, jax.random.fold_in(stream_key, 6)
    for dim, shards_of in shards:
        draws = jnp.exp(jax.random.uniform(jax.random.fold_in(own, dim), (shards_of,), jnp.float32, smallest / len(shards), top_value / len(shards)))
        loudness = loudness * jnp.repeat(draws, extent[dim] // shards_of).reshape([-1 if axis == dim else 1 for axis in range(len(extent))])
    return loudness


def centred(own_key, shape, spread, most, cuts=(), kind=jnp.bfloat16):
    gain = steps_of(own_key, shape, cuts, -0.22, 0.18) if cuts else 1.0
    result = jax.random.normal(own_key, shape, jnp.float32) * spread * gain
    return jnp.minimum(jnp.maximum(result, -most), most).astype(kind)


def setup_inputs(seed: int = 0) -> dict:
    arg_keys = jax.random.split(jax.random.key(seed), 6)
    start_block = centred(arg_keys[0], (K, NV), 1.0, 6.0, ((1, 128),), jnp.float32)
    blocks = draw_blocks(jax.random.fold_in(arg_keys[5], 71), 0)
    block_rows = draw_block_rows(jax.random.fold_in(arg_keys[5], 71), 0)
    block_cols = draw_block_cols(jax.random.fold_in(arg_keys[5], 71), 0)
    counts = draw_counts(jax.random.fold_in(arg_keys[5], 71), 0)
    return dict(start_block=start_block, blocks=blocks, block_rows=block_rows, block_cols=block_cols, counts=counts)


def product(half, blocks, block_rows, block_cols, counts):
    vectors = half.shape[0]
    whole = half.astype(jnp.float32).reshape(vectors, N_ROW, N_COL, VP)
    row_blocks = N_COL * M
    col_blocks = N_ROW * M
    slot_ids = jnp.arange(MAXB, dtype=jnp.int32)

    def visit(tile_index, total):
        tile_row = (tile_index // N_COL).astype(jnp.int32)
        tile_col = (tile_index % N_COL).astype(jnp.int32)
        tile_data = blocks[tile_row, tile_col].astype(jnp.float32)
        row_ids = block_rows[tile_row, tile_col].astype(jnp.int32)
        col_ids = block_cols[tile_row, tile_col].astype(jnp.int32)
        is_live = slot_ids < counts[tile_row, tile_col]
        row_vector = lax.dynamic_index_in_dim(whole, tile_row, 1, False).reshape(vectors, row_blocks, BS)
        col_vector = lax.dynamic_index_in_dim(whole, tile_col, 2, False).reshape(vectors, col_blocks, BS)
        global_row = tile_row * row_blocks + row_ids
        global_col = (col_ids // M * N_COL + tile_col) * M + col_ids % M
        mirror = is_live & (global_row != global_col)
        direct = jnp.einsum('gij,kgj->kgi', tile_data, col_vector[:, col_ids])
        turned = jnp.einsum('gji,kgj->kgi', tile_data, row_vector[:, row_ids])
        direct = jnp.where(is_live[None, :, None], direct, 0.0)
        turned = jnp.where(mirror[None, :, None], turned, 0.0)
        row_out = jnp.zeros((vectors, row_blocks, BS), jnp.float32).at[:, row_ids].add(direct)
        col_out = jnp.zeros((vectors, col_blocks, BS), jnp.float32).at[:, col_ids].add(turned)
        row_now = lax.dynamic_index_in_dim(total, tile_row, 1, False) + row_out.reshape(vectors, N_COL, VP)
        total = lax.dynamic_update_index_in_dim(total, row_now, tile_row, 1)
        col_now = lax.dynamic_index_in_dim(total, tile_col, 2, False) + col_out.reshape(vectors, N_ROW, VP)
        total = lax.dynamic_update_index_in_dim(total, col_now, tile_col, 2)
        return total
    total = lax.fori_loop(0, N_ROW * N_COL, visit, jnp.zeros((vectors, N_ROW, N_COL, VP), jnp.float32))
    return total.reshape(vectors, N_ROW * N_COL * VP)

def reference(start_block, blocks, block_rows, block_cols, counts):
    highest = lax.Precision.HIGHEST
    factor = jnp.linalg.cholesky(jnp.dot(start_block, start_block.T, precision=highest))
    current = lax.linalg.triangular_solve(factor, start_block, left_side=True, lower=True)
    previous = current
    prev_factor = factor
    diagonals = []
    couplings = []
    for step_index in range(ITERS):
        image = product(current.astype(jnp.bfloat16), blocks, block_rows, block_cols, counts)
        if step_index > 0:
            image = image - jnp.dot(prev_factor.T, previous, precision=highest)
        projection = jnp.dot(current, image.T, precision=highest)
        image = image - jnp.dot(projection.T, current, precision=highest)
        gram = jnp.dot(image, image.T, precision=highest)
        factor = jnp.linalg.cholesky(gram)
        following = lax.linalg.triangular_solve(factor, image, left_side=True, lower=True)
        diagonals.append(projection)
        couplings.append(factor)
        previous, prev_factor, current = (current, factor, following)
    tri_size = ITERS * K
    tridiagonal = jnp.zeros((tri_size, tri_size), jnp.float32)
    for step_index in range(ITERS):
        low = step_index * K
        tridiagonal = tridiagonal.at[low:low + K, low:low + K].set(diagonals[step_index])
        if step_index + 1 < ITERS:
            tridiagonal = tridiagonal.at[low:low + K, low + K:low + 2 * K].set(couplings[step_index])
            tridiagonal = tridiagonal.at[low + K:low + 2 * K, low:low + K].set(couplings[step_index].T)
    return (current * jnp.sqrt(jnp.float32(NV)), tridiagonal)
```

```python
import functools
import math

import jax
import jax.numpy as jnp
from jax import lax
from jax.experimental import pallas as pl
from jax.experimental.pallas import tpu as pltpu
from jax.sharding import PartitionSpec as P

F32 = jnp.float32
BF16 = jnp.bfloat16
MESH = pl.DeviceIdType.MESH

K = 8
LANES = 128
M = 8
SIDE = 4
NR, NC = 16, 8
RB, CB = NC * M, NR * M
SLOTS = 128
BATCH = 4


def bcast(x):
    return jnp.broadcast_to(x, (K, LANES))


def kernel(
    x_in, blocks, rows_s, cols_s, counts_s, rows_v, cols_v,
    next_out, tri_out,
    bl, xb, yb, xall, yall, picks_r, picks_c, res_d, res_t,
    tot_r, tot_c, in_r, in_c, ykb, qown, wbuf,
    msg, msg2, ar_r, ar_c,
    load_sem, send_sem, recv_sem,
):
    r = lax.axis_index("row")
    c = lax.axis_index("col")
    row_iota = lax.broadcasted_iota(jnp.int32, (K, LANES), 0)
    lane_iota = lax.broadcasted_iota(jnp.int32, (K, LANES), 1)

    row_peers = []
    z0, x0 = r // SIDE, lax.rem(r, SIDE)
    for off in range(1, NR):
        dz, dx = off // SIDE, off % SIDE
        row_peers.append(lax.rem(z0 + dz, SIDE) * SIDE + lax.rem(x0 + dx, SIDE))
    col_peers = []
    y0, p0 = c // 2, lax.rem(c, 2)
    for off in range(1, NC):
        dy, dp = off // 2, off % 2
        col_peers.append(lax.rem(y0 + dy, SIDE) * 2 + lax.rem(p0 + dp, 2))

    barrier = pltpu.get_barrier_semaphore()
    for rr in row_peers:
        pl.semaphore_signal(barrier, inc=1, device_id=(rr, c), device_id_type=MESH)
    for cc in col_peers:
        pl.semaphore_signal(barrier, inc=1, device_id=(r, cc), device_id_type=MESH)

    parts = 4
    step = SLOTS // parts
    loads = [
        pltpu.make_async_copy(
            blocks.at[0, 0, pl.ds(i * step, step)], bl.at[pl.ds(i * step, step)], load_sem.at[i]
        )
        for i in range(parts)
    ]
    for load in loads:
        load.start()

    def send(src, dst, sems, dev):
        pltpu.make_async_remote_copy(
            src_ref=src, dst_ref=dst, send_sem=send_sem.at[sems], recv_sem=recv_sem.at[sems],
            device_id=dev, device_id_type=MESH,
        ).start()

    def wait_bytes(ref, sem):
        pltpu.make_async_copy(ref, ref, sem).wait()

    def gram(a_ref, b_ref, lane0, tile):
        for j in range(K):
            acc = None
            for b in range(M):
                term = a_ref[b] * b_ref[b, pl.ds(j, 1), :]
                acc = term if acc is None else acc + term
            col = jnp.sum(acc, axis=1, keepdims=True)
            tile = jnp.where(lane_iota == lane0 + j, bcast(col), tile)
        return tile

    def reduce_rows_start(n, tile):
        msg[n] = tile
        for rr in row_peers:
            send(msg.at[n], ar_r.at[n, r], 6 * n + 0, (rr, c))

    def reduce_finish(n):
        wait_bytes(ar_r.at[n, pl.ds(0, NR - 1)], recv_sem.at[6 * n + 0])
        ar_r[n, r] = msg[n]
        total = ar_r[n, 0]
        for i in range(1, NR):
            total = total + ar_r[n, i]
        msg2[n] = total
        for cc in col_peers:
            send(msg2.at[n], ar_c.at[n, c], 6 * n + 1, (r, cc))
        wait_bytes(ar_c.at[n, pl.ds(0, NC - 1)], recv_sem.at[6 * n + 1])
        ar_c[n, c] = msg2[n]
        total = ar_c[n, 0]
        for i in range(1, NC):
            total = total + ar_c[n, i]
        return total

    def columns(tile, lane0):
        return [bcast(tile[:, lane0 + j : lane0 + j + 1]) for j in range(K)]

    def factor(gcols):
        g = list(gcols)
        d = [jnp.where(row_iota == m, 1.0, 0.0).astype(F32) for m in range(K)]
        unit = []
        diag = g[0]
        for j in range(K):
            inv = 1.0 / g[j][j : j + 1, :]
            f = jnp.where(row_iota > j, g[j] * inv, 0.0)
            unit.append(f + jnp.where(row_iota == j, 1.0, 0.0))
            if j:
                diag = jnp.where(row_iota == j, g[j], diag)
            for m in range(j + 1, K):
                g[m] = g[m] - f * g[m][j : j + 1, :]
            for m in range(j + 1):
                d[m] = d[m] - f * d[m][j : j + 1, :]
        root = jnp.sqrt(diag)
        rs = 1.0 / root
        inverse = [v * rs for v in d]
        upper = [jnp.where(row_iota <= m, g[m], 0.0) * rs for m in range(K)]
        lower = [unit[j] * root[j : j + 1, :] for j in range(K)]
        return inverse, upper, lower

    def matmul_cols(left, right):
        out = []
        for m in range(K):
            acc = left[0] * right[m][0:1, :]
            for p in range(1, K):
                acc = acc + left[p] * right[m][p : p + 1, :]
            out.append(acc)
        return out

    def apply(cols, ref, i):
        acc = cols[0] * ref[i, pl.ds(0, 1), :]
        for j in range(1, K):
            acc = acc + cols[j] * ref[i, pl.ds(j, 1), :]
        return acc

    def gather_start(src, dst, n):
        for rr in row_peers:
            send(src, dst.at[pl.ds(RB + M * r, M)], 6 * n + 2, (rr, c))
        for cc in col_peers:
            send(src, dst.at[pl.ds(M * c, M)], 6 * n + 3, (r, cc))

    def gather_finish(src, dst, n):
        for b in range(M):
            dst[RB + M * r + b] = src[b]
            dst[M * c + b] = src[b]
        wait_bytes(dst.at[pl.ds(0, (NR - 1) * M)], recv_sem.at[6 * n + 2])
        wait_bytes(dst.at[pl.ds(0, (NC - 1) * M)], recv_sem.at[6 * n + 3])

    zero = jnp.zeros((K, LANES), F32)

    def cat(a, b, axis):
        return jnp.concatenate([a, b], axis=axis)

    def product(vec):
        def body(q, carry):
            base = BATCH * q
            b = [bl[base + i] for i in range(BATCH)]
            tile = cat(cat(b[0], b[1], 0), cat(b[2], b[3], 0), 1)
            xr = [vec[rows_s[r, 0, base + i]] for i in range(BATCH)]
            xc = [vec[RB + cols_s[r, 0, base + i]] for i in range(BATCH)]
            lhs_t = jnp.concatenate(
                [cat(xr[0], zero, 1), cat(zero, xr[1], 1), cat(xr[2], zero, 1), cat(zero, xr[3], 1)],
                axis=0,
            ).astype(BF16)
            lhs_d = jnp.concatenate(
                [cat(xc[0], zero, 1), cat(xc[1], zero, 1), cat(zero, xc[2], 1), cat(zero, xc[3], 1)],
                axis=0,
            ).astype(BF16)
            turned = lax.dot_general(
                lhs_t, tile, (((1,), (0,)), ((), ())), preferred_element_type=F32
            )
            direct = lax.dot_general(
                lhs_d, tile, (((1,), (1,)), ((), ())), preferred_element_type=F32
            )
            for i in range(BATCH):
                ht = i // 2
                hd = i % 2
                res_t[pl.ds(base + i, K, stride=SLOTS), :] = turned[
                    K * i : K * i + K, LANES * ht : LANES * ht + LANES
                ]
                res_d[pl.ds(base + i, K, stride=SLOTS), :] = direct[
                    K * i : K * i + K, LANES * hd : LANES * hd + LANES
                ]
            return carry

        lax.fori_loop(0, SLOTS // BATCH, body, 0, unroll=2)

    def scatter(pick, res, tot, pieces):
        for kk in range(K // 2):
            full = cat(
                res[pl.ds(2 * kk * SLOTS, SLOTS), :], res[pl.ds((2 * kk + 1) * SLOTS, SLOTS), :], 1
            )
            hi = full.astype(BF16)
            lo = (full - hi.astype(F32)).astype(BF16)
            out = jnp.dot(pick[...], cat(hi, lo, 0), preferred_element_type=F32)
            for i in range(pieces):
                for h in range(2):
                    tot[i, 2 * kk + h] = out[M * i : M * i + M, LANES * h : LANES * h + LANES]

    def reduce_scatter(n, out_ref):
        for i, rr in enumerate(row_peers):
            send(tot_c.at[n, rr], in_c.at[n, r], 6 * n + 4, (rr, c))
        for i, cc in enumerate(col_peers):
            send(tot_r.at[n, cc], in_r.at[n, c], 6 * n + 5, (r, cc))
        in_c[n, r] = tot_c[n, r]
        in_r[n, c] = tot_r[n, c]
        wait_bytes(in_c.at[n, pl.ds(0, NR - 1)], recv_sem.at[6 * n + 4])
        wait_bytes(in_r.at[n, pl.ds(0, NC - 1)], recv_sem.at[6 * n + 5])
        for k in range(K):
            total = in_c[n, 0, k]
            for i in range(1, NR):
                total = total + in_c[n, i, k]
            for i in range(NC):
                total = total + in_r[n, i, k]
            ykb[pl.ds(M * k, M), :] = total
        for b in range(M):
            out_ref[b] = ykb[pl.ds(b, K, stride=M), :]

    for b in range(M):
        xb[b] = x_in[:, pl.ds(LANES * b, LANES)]
    start_tile = gram(xb, xb, 0, zero)

    giota = lax.broadcasted_iota(jnp.int32, (1, SLOTS), 1)
    row_ids = rows_v[r]
    col_ids = cols_v[r]
    valid = giota < counts_s[r, c]
    global_row = r * RB + row_ids
    global_col = ((col_ids // M) * NC + c) * M + lax.rem(col_ids, M)
    mirror = jnp.logical_and(valid, global_row != global_col)
    want_r = jnp.where(valid, row_ids, -1)
    want_c = jnp.where(mirror, col_ids, -1)
    one_r = jnp.where(lax.broadcasted_iota(jnp.int32, (RB, SLOTS), 0) == want_r, 1.0, 0.0)
    one_c = jnp.where(lax.broadcasted_iota(jnp.int32, (CB, SLOTS), 0) == want_c, 1.0, 0.0)
    one_r = one_r.astype(BF16)
    one_c = one_c.astype(BF16)
    picks_r[...] = cat(one_r, one_r, 1)
    picks_c[...] = cat(one_c, one_c, 1)

    pl.semaphore_wait(barrier, NR + NC - 2)

    reduce_rows_start(0, start_tile)
    gather_start(xb, xall, 0)
    inverse, _, _ = factor(columns(reduce_finish(0), 0))
    gather_finish(xb, xall, 0)

    def normalise(i, carry):
        for u in range(8):
            t = 8 * i + u
            xall[t] = apply(inverse, xall, t)
        return carry

    lax.fori_loop(0, (RB + CB) // 8, normalise, 0)
    for load in loads:
        load.wait()
    product(xall)
    scatter(picks_r, res_d, tot_r.at[0], NC)
    scatter(picks_c, res_t, tot_c.at[0], NR)
    reduce_scatter(0, yb)

    for b in range(M):
        qown[0, b] = xall[M * c + b]
    tile = gram(yb, qown.at[0], 0, zero)
    tile = gram(yb, yb, K, tile)
    tile = gram(qown.at[0], yb, 2 * K, tile)
    reduce_rows_start(1, tile)
    gather_start(yb, yall, 1)
    total = reduce_finish(1)
    at_cols = columns(total, 0)
    s_cols = columns(total, K)
    a1_cols = columns(total, 2 * K)
    ata = matmul_cols(at_cols, a1_cols)
    inverse, upper1, lower1 = factor([s - t for s, t in zip(s_cols, ata)])
    back = matmul_cols(inverse, at_cols)
    gather_finish(yb, yall, 1)

    def advance(i, carry):
        for u in range(4):
            t = 4 * i + u
            yall[t] = apply(inverse, yall, t) - apply(back, xall, t)
        return carry

    lax.fori_loop(0, (RB + CB) // 4, advance, 0)
    product(yall)
    scatter(picks_r, res_d, tot_r.at[1], NC)
    scatter(picks_c, res_t, tot_c.at[1], NR)
    reduce_scatter(1, wbuf)
    for b in range(M):
        qown[1, b] = yall[M * c + b]
        wbuf[b] = wbuf[b] - apply(upper1, qown.at[0], b)
    tile = gram(wbuf, qown.at[1], 0, zero)
    tile = gram(wbuf, wbuf, K, tile)
    tile = gram(qown.at[1], wbuf, 2 * K, tile)
    reduce_rows_start(2, tile)
    total = reduce_finish(2)
    at_cols = columns(total, 0)
    s_cols = columns(total, K)
    a2_cols = columns(total, 2 * K)
    ata = matmul_cols(at_cols, a2_cols)
    inverse, _, _ = factor([s - t for s, t in zip(s_cols, ata)])
    back = matmul_cols(inverse, at_cols)
    order_root = math.sqrt(NR * NC * M * LANES)
    for b in range(M):
        value = apply(inverse, wbuf, b) - apply(back, qown.at[1], b)
        next_out[:, pl.ds(LANES * b, LANES)] = value * order_root
    top = zero
    low = zero
    for j in range(K):
        top = jnp.where(lane_iota == j, a1_cols[j], top)
        top = jnp.where(lane_iota == K + j, lower1[j], top)
        low = jnp.where(lane_iota == j, upper1[j], low)
        low = jnp.where(lane_iota == K + j, a2_cols[j], low)
    tri_out[pl.ds(0, K), :] = top[:, : 2 * K]
    tri_out[pl.ds(K, K), :] = low[:, : 2 * K]

    for n in range(3):
        wait_bytes(ar_r.at[n, pl.ds(0, NR - 1)], send_sem.at[6 * n + 0])
        wait_bytes(ar_c.at[n, pl.ds(0, NC - 1)], send_sem.at[6 * n + 1])
    for n in range(2):
        wait_bytes(xall.at[pl.ds(0, (NR - 1) * M)], send_sem.at[6 * n + 2])
        wait_bytes(xall.at[pl.ds(0, (NC - 1) * M)], send_sem.at[6 * n + 3])
        wait_bytes(in_c.at[n, pl.ds(0, NR - 1)], send_sem.at[6 * n + 4])
        wait_bytes(in_r.at[n, pl.ds(0, NC - 1)], send_sem.at[6 * n + 5])


def per_device(start_block, blocks, block_rows, block_cols, counts):
    vmem = pl.BlockSpec(memory_space=pltpu.VMEM)
    smem = pl.BlockSpec(memory_space=pltpu.SMEM)
    tile = (K, LANES)
    return pl.pallas_call(
        kernel,
        out_shape=(
            jax.ShapeDtypeStruct((K, M * LANES), F32),
            jax.ShapeDtypeStruct((2 * K, 2 * K), F32),
        ),
        in_specs=[vmem, pl.BlockSpec(memory_space=pl.ANY), smem, smem, smem, vmem, vmem],
        out_specs=(vmem, vmem),
        scratch_shapes=[
            pltpu.VMEM((SLOTS, LANES, LANES), BF16),
            pltpu.VMEM((M, *tile), F32),
            pltpu.VMEM((M, *tile), F32),
            pltpu.VMEM((RB + CB, *tile), F32),
            pltpu.VMEM((RB + CB, *tile), F32),
            pltpu.VMEM((RB, 2 * SLOTS), BF16),
            pltpu.VMEM((CB, 2 * SLOTS), BF16),
            pltpu.VMEM((K * SLOTS, LANES), F32),
            pltpu.VMEM((K * SLOTS, LANES), F32),
            pltpu.VMEM((2, NC, K, M, LANES), F32),
            pltpu.VMEM((2, NR, K, M, LANES), F32),
            pltpu.VMEM((2, NC, K, M, LANES), F32),
            pltpu.VMEM((2, NR, K, M, LANES), F32),
            pltpu.VMEM((K * M, LANES), F32),
            pltpu.VMEM((2, M, *tile), F32),
            pltpu.VMEM((M, *tile), F32),
            pltpu.VMEM((3, *tile), F32),
            pltpu.VMEM((3, *tile), F32),
            pltpu.VMEM((3, NR, *tile), F32),
            pltpu.VMEM((3, NC, *tile), F32),
            pltpu.SemaphoreType.DMA((4,)),
            pltpu.SemaphoreType.DMA((18,)),
            pltpu.SemaphoreType.DMA((18,)),
        ],
        compiler_params=pltpu.CompilerParams(
            collective_id=0, has_side_effects=True, vmem_limit_bytes=48 * 1024 * 1024
        ),
        name="lanczos",
    )(start_block, blocks, block_rows, block_cols, counts, block_rows, block_cols)


def solution(mesh):
    assert mesh.shape["row"] == NR and mesh.shape["col"] == NC
    both = ("row", "col")
    return jax.shard_map(
        per_device,
        mesh=mesh,
        in_specs=(
            P(None, both),
            P("row", "col", None, None, None),
            P(None, "col", None),
            P(None, "col", None),
            P(),
        ),
        out_specs=(P(None, both), P()),
        check_vma=False,
    )
```

```python
import functools
import math

import jax
import jax.numpy as jnp
from jax import lax
from jax.experimental import pallas as pl
from jax.experimental.pallas import tpu as pltpu
from jax.sharding import PartitionSpec as P

F32 = jnp.float32
BF16 = jnp.bfloat16
MESH = pl.DeviceIdType.MESH

K = 8
LANES = 128
M = 8
SIDE = 4
NR, NC = 16, 8
RB, CB = NC * M, NR * M
SLOTS = 128
BATCH = 4
UNROLL = 16
SUM_C = BF16
SUM_R = BF16


def bcast(x):
    return jnp.broadcast_to(x, (K, LANES))


def kernel(
    x_hbm, blocks, rows_hbm, cols_hbm, counts_hbm,
    next_out, tri_out,
    bl, x_in, rows_s, cols_s, counts_s, rows_v, cols_v, xb, yb, xr, xc, yr, yc, picks_r, picks_c, res_d, res_t,
    tot_r, tot_c, in_r, in_c, ykb, qown, wbuf, msg, ar,
    load_sem, send_sem, recv_sem,
):
    r = lax.axis_index("row")
    c = lax.axis_index("col")
    row_iota = lax.broadcasted_iota(jnp.int32, (K, LANES), 0)
    lane_iota = lax.broadcasted_iota(jnp.int32, (K, LANES), 1)

    row_peers = []
    z0, x0 = r // SIDE, lax.rem(r, SIDE)
    for off in range(1, NR):
        dz, dx = off // SIDE, off % SIDE
        row_peers.append(lax.rem(z0 + dz, SIDE) * SIDE + lax.rem(x0 + dx, SIDE))
    col_peers = []
    y0, p0 = c // 2, lax.rem(c, 2)
    for off in range(1, NC):
        dy, dp = off // 2, off % 2
        col_peers.append(lax.rem(y0 + dy, SIDE) * 2 + lax.rem(p0 + dp, 2))

    others = [(rr, cc) for cc in [c] + col_peers for rr in [r] + row_peers][1:]
    others = others[::-1]

    barrier = pltpu.get_barrier_semaphore()
    for dev in others:
        pl.semaphore_signal(barrier, inc=1, device_id=dev, device_id_type=MESH)

    parts = 4
    step = SLOTS // parts
    loads = [
        pltpu.make_async_copy(
            blocks.at[0, 0, pl.ds(i * step, step)], bl.at[pl.ds(i * step, step)], load_sem.at[i]
        )
        for i in range(parts)
    ]
    small = [
        pltpu.make_async_copy(src, dst, load_sem.at[parts + i])
        for i, (src, dst) in enumerate(
            [
                (x_hbm, x_in),
                (rows_hbm.at[r], rows_s),
                (cols_hbm.at[r], cols_s),
                (counts_hbm, counts_s),
                (rows_hbm.at[r], rows_v),
                (cols_hbm.at[r], cols_v),
            ]
        )
    ]
    for load in small + loads:
        load.start()

    def send(src, dst, sems, dev):
        pltpu.make_async_remote_copy(
            src_ref=src, dst_ref=dst, send_sem=send_sem.at[sems], recv_sem=recv_sem.at[sems],
            device_id=dev, device_id_type=MESH,
        ).start()

    def wait_bytes(ref, sem):
        pltpu.make_async_copy(ref, ref, sem).wait()

    def gram(a_ref, b_ref, lane0, tile):
        for j in range(K):
            acc = None
            for b in range(M):
                term = a_ref[b] * b_ref[b, pl.ds(j, 1), :]
                acc = term if acc is None else acc + term
            col = jnp.sum(acc, axis=1, keepdims=True)
            tile = jnp.where(lane_iota == 2 * K * row_iota + (lane0 + j), bcast(col), tile)
        return tile

    def reduce_start(n, tile):
        msg[n] = jnp.sum(tile, axis=0, keepdims=True)
        for dev in others:
            send(msg.at[n], ar.at[n, r * NC + c], 6 * n, dev)

    def reduce_finish(n):
        wait_bytes(ar.at[n, pl.ds(0, NR * NC - 1)], recv_sem.at[6 * n])
        ar[n, r * NC + c] = msg[n]
        sums = [ar[n, i] for i in range(8)]
        for i in range(8, NR * NC):
            sums[i % 8] = sums[i % 8] + ar[n, i]
        while len(sums) > 1:
            sums = [p + q for p, q in zip(sums[::2], sums[1::2])]
        return bcast(sums[0])

    def picked(total, lanes):
        return bcast(jnp.sum(jnp.where(lane_iota == lanes, total, 0.0), axis=1, keepdims=True))

    def columns(total, lane0):
        return [picked(total, 2 * K * row_iota + (lane0 + j)) for j in range(K)]

    def rows_of(total):
        return [picked(total, row_iota + 2 * K * j) for j in range(K)]

    def factor(gcols):
        g = list(gcols)
        d = [jnp.where(row_iota == m, 1.0, 0.0).astype(F32) for m in range(K)]
        unit = []
        diag = g[0]
        for j in range(K):
            inv = 1.0 / g[j][j : j + 1, :]
            f = jnp.where(row_iota > j, g[j] * inv, 0.0)
            unit.append(f + jnp.where(row_iota == j, 1.0, 0.0))
            if j:
                diag = jnp.where(row_iota == j, g[j], diag)
            for m in range(j + 1, K):
                g[m] = g[m] - f * g[m][j : j + 1, :]
            for m in range(j + 1):
                d[m] = d[m] - f * d[m][j : j + 1, :]
        root = jnp.sqrt(diag)
        rs = 1.0 / root
        inverse = [v * rs for v in d]
        upper = [jnp.where(row_iota <= m, g[m], 0.0) * rs for m in range(K)]
        lower = [unit[j] * root[j : j + 1, :] for j in range(K)]
        return inverse, upper, lower

    def matmul_cols(left, right):
        out = []
        for m in range(K):
            acc = left[0] * right[m][0:1, :]
            for p in range(1, K):
                acc = acc + left[p] * right[m][p : p + 1, :]
            out.append(acc)
        return out

    def apply(cols, ref, i):
        acc = cols[0] * ref[i, pl.ds(0, 1), :]
        for j in range(1, K):
            acc = acc + cols[j] * ref[i, pl.ds(j, 1), :]
        return acc

    def gather_start(src, seg_r, seg_c, n):
        for cc in col_peers:
            send(src, seg_r.at[pl.ds(M * c, M)], 6 * n + 3, (r, cc))
        for rr in row_peers:
            send(src, seg_c.at[pl.ds(M * r, M)], 6 * n + 2, (rr, c))
        for b in range(M):
            seg_c[M * r + b] = src[b]
            seg_r[M * c + b] = src[b]

    def gather_wait_col(seg_r, n):
        wait_bytes(seg_r.at[pl.ds(0, (NC - 1) * M)], recv_sem.at[6 * n + 3])

    def gather_wait_row(seg_c, n):
        wait_bytes(seg_c.at[pl.ds(0, (NR - 1) * M)], recv_sem.at[6 * n + 2])

    zero = jnp.zeros((K, LANES), F32)

    def cat(a, b, axis):
        return jnp.concatenate([a, b], axis=axis)

    def product(vec, ids, turn, res):
        def body(q, carry):
            base = BATCH * q
            b = [bl[base + i] for i in range(BATCH)]
            tile = cat(cat(b[0], b[1], 0), cat(b[2], b[3], 0), 1)
            x = [vec[ids[0, base + i]] for i in range(BATCH)]
            depth = [i % 2 if turn else i // 2 for i in range(BATCH)]
            width = [i // 2 if turn else i % 2 for i in range(BATCH)]
            lhs = jnp.concatenate(
                [cat(zero, x[i], 1) if depth[i] else cat(x[i], zero, 1) for i in range(BATCH)],
                axis=0,
            ).astype(BF16)
            out = lax.dot_general(
                lhs, tile, (((1,), (0 if turn else 1,)), ((), ())), preferred_element_type=F32
            )
            for i in range(BATCH):
                res[pl.ds(base + i, K, stride=SLOTS), :] = out[
                    K * i : K * i + K, LANES * width[i] : LANES * width[i] + LANES
                ]
            return carry

        lax.fori_loop(0, SLOTS // BATCH, body, 0, unroll=UNROLL)

    def scatter(pick, res, put):
        for kk in range(K // 2):
            full = cat(
                res[pl.ds(2 * kk * SLOTS, SLOTS), :], res[pl.ds((2 * kk + 1) * SLOTS, SLOTS), :], 1
            )
            hi = full.astype(BF16)
            lo = (full - hi.astype(F32)).astype(BF16)
            put(kk, jnp.dot(pick[...], cat(hi, lo, 0), preferred_element_type=F32))

    def exchange_cols(n):
        def put(kk, out):
            for i in range(NR):
                rows = out[M * i : M * i + M]
                tot_c[n, i, kk] = cat(rows[:, :LANES], rows[:, LANES:], 0).astype(tot_c.dtype)

        scatter(picks_c, res_t, put)
        for rr in row_peers:
            send(tot_c.at[n, rr], in_c.at[n, r], 6 * n + 4, (rr, c))
        in_c[n, r] = tot_c[n, r]

    def exchange_rows(n):
        def put(kk, out):
            for i in range(NC):
                rows = out[M * i : M * i + M]
                tot_r[n, i, kk] = cat(rows[:, :LANES], rows[:, LANES:], 0).astype(tot_r.dtype)

        scatter(picks_r, res_d, put)
        for cc in col_peers:
            send(tot_r.at[n, cc], in_r.at[n, c], 6 * n + 5, (r, cc))
        in_r[n, c] = tot_r[n, c]

    def exchange_finish(n, out_ref):
        wait_bytes(in_r.at[n, pl.ds(0, NC - 1)], recv_sem.at[6 * n + 5])
        for kk in range(K // 2):
            total = in_r[n, 0, kk].astype(F32)
            for i in range(1, NC):
                total = total + in_r[n, i, kk].astype(F32)
            ykb[pl.ds(2 * M * kk, 2 * M), :] = total
        wait_bytes(in_c.at[n, pl.ds(0, NR - 1)], recv_sem.at[6 * n + 4])
        for kk in range(K // 2):
            total = ykb[pl.ds(2 * M * kk, 2 * M), :]
            for i in range(NR):
                total = total + in_c[n, i, kk].astype(F32)
            ykb[pl.ds(2 * M * kk, 2 * M), :] = total
        for b in range(M):
            out_ref[b] = ykb[pl.ds(b, K, stride=M), :]

    def sweep(count, step, update):
        def body(i, carry):
            for u in range(step):
                update(step * i + u)
            return carry

        lax.fori_loop(0, count // step, body, 0)

    for load in small:
        load.wait()
    for b in range(M):
        xb[b] = x_in[:, pl.ds(LANES * b, LANES)]
    start_tile = gram(xb, xb, 0, zero)

    giota = lax.broadcasted_iota(jnp.int32, (1, SLOTS), 1)
    row_ids = rows_v[...]
    col_ids = cols_v[...]
    valid = giota < counts_s[c, r]
    global_row = r * RB + row_ids
    global_col = ((col_ids // M) * NC + c) * M + lax.rem(col_ids, M)
    mirror = jnp.logical_and(valid, global_row != global_col)
    want_r = jnp.where(valid, row_ids, -1)
    want_c = jnp.where(mirror, col_ids, -1)
    one_r = jnp.where(lax.broadcasted_iota(jnp.int32, (RB, SLOTS), 0) == want_r, 1.0, 0.0)
    one_c = jnp.where(lax.broadcasted_iota(jnp.int32, (CB, SLOTS), 0) == want_c, 1.0, 0.0)
    one_r = one_r.astype(BF16)
    one_c = one_c.astype(BF16)
    picks_r[...] = cat(one_r, one_r, 1)
    picks_c[...] = cat(one_c, one_c, 1)

    pl.semaphore_wait(barrier, NR * NC - 1)

    reduce_start(0, start_tile)
    gather_start(xb, xr, xc, 0)
    inverse, _, _ = factor(columns(reduce_finish(0), 0))

    def normalise(seg, t):
        seg[t] = apply(inverse, seg, t)

    gather_wait_col(xr, 0)
    sweep(RB, 8, functools.partial(normalise, xr))
    for load in loads:
        load.wait()
    product(xr, rows_s, True, res_t)
    exchange_cols(0)
    gather_wait_row(xc, 0)
    sweep(CB, 8, functools.partial(normalise, xc))
    product(xc, cols_s, False, res_d)
    exchange_rows(0)
    for b in range(M):
        qown[0, b] = xr[M * c + b]
    exchange_finish(0, yb)

    tile = gram(yb, qown.at[0], 0, zero)
    tile = gram(yb, yb, K, tile)
    reduce_start(1, tile)
    gather_start(yb, yr, yc, 1)
    total = reduce_finish(1)
    at_cols = columns(total, 0)
    s_cols = columns(total, K)
    a1_cols = rows_of(total)
    ata = matmul_cols(at_cols, a1_cols)
    inverse, upper1, lower1 = factor([s - t for s, t in zip(s_cols, ata)])
    back = matmul_cols(inverse, at_cols)

    def advance(seg, old, t):
        seg[t] = apply(inverse, seg, t) - apply(back, old, t)

    gather_wait_col(yr, 1)
    sweep(RB, 4, functools.partial(advance, yr, xr))
    product(yr, rows_s, True, res_t)
    exchange_cols(1)
    gather_wait_row(yc, 1)
    sweep(CB, 4, functools.partial(advance, yc, xc))
    product(yc, cols_s, False, res_d)
    exchange_rows(1)
    for b in range(M):
        qown[1, b] = yr[M * c + b]
    top = zero
    for j in range(K):
        top = jnp.where(lane_iota == j, a1_cols[j], top)
        top = jnp.where(lane_iota == K + j, lower1[j], top)
    tri_out[pl.ds(0, K), :] = top[:, : 2 * K]
    exchange_finish(1, wbuf)
    for b in range(M):
        wbuf[b] = wbuf[b] - apply(upper1, qown.at[0], b)
    tile = gram(wbuf, qown.at[1], 0, zero)
    tile = gram(wbuf, wbuf, K, tile)
    reduce_start(2, tile)

    for n in range(2):
        wait_bytes(ar.at[n, pl.ds(0, NR * NC - 1)], send_sem.at[6 * n])
        wait_bytes(xc.at[pl.ds(0, (NR - 1) * M)], send_sem.at[6 * n + 2])
        wait_bytes(xr.at[pl.ds(0, (NC - 1) * M)], send_sem.at[6 * n + 3])
        wait_bytes(in_c.at[n, pl.ds(0, NR - 1)], send_sem.at[6 * n + 4])
        wait_bytes(in_r.at[n, pl.ds(0, NC - 1)], send_sem.at[6 * n + 5])

    total = reduce_finish(2)
    at_cols = columns(total, 0)
    s_cols = columns(total, K)
    a2_cols = rows_of(total)
    ata = matmul_cols(at_cols, a2_cols)
    inverse, _, _ = factor([s - t for s, t in zip(s_cols, ata)])
    back = matmul_cols(inverse, at_cols)
    order_root = math.sqrt(NR * NC * M * LANES)
    for b in range(M):
        value = apply(inverse, wbuf, b) - apply(back, qown.at[1], b)
        next_out[:, pl.ds(LANES * b, LANES)] = value * order_root
    low = zero
    for j in range(K):
        low = jnp.where(lane_iota == j, upper1[j], low)
        low = jnp.where(lane_iota == K + j, a2_cols[j], low)
    tri_out[pl.ds(K, K), :] = low[:, : 2 * K]
    wait_bytes(ar.at[2, pl.ds(0, NR * NC - 1)], send_sem.at[12])


def per_device(start_block, blocks, block_rows, block_cols, counts):
    vmem = pl.BlockSpec(memory_space=pltpu.VMEM)
    hbm = pl.BlockSpec(memory_space=pltpu.HBM)
    tile = (K, LANES)
    return pl.pallas_call(
        kernel,
        out_shape=(
            jax.ShapeDtypeStruct((K, M * LANES), F32),
            jax.ShapeDtypeStruct((2 * K, 2 * K), F32),
        ),
        in_specs=[hbm] * 5,
        out_specs=(vmem, vmem),
        scratch_shapes=[
            pltpu.VMEM((SLOTS, LANES, LANES), BF16),
            pltpu.VMEM((K, M * LANES), F32),
            pltpu.SMEM((1, SLOTS), jnp.int32),
            pltpu.SMEM((1, SLOTS), jnp.int32),
            pltpu.SMEM((NC, NR), jnp.int32),
            pltpu.VMEM((1, SLOTS), jnp.int32),
            pltpu.VMEM((1, SLOTS), jnp.int32),
            pltpu.VMEM((M, *tile), F32),
            pltpu.VMEM((M, *tile), F32),
            pltpu.VMEM((RB, *tile), F32),
            pltpu.VMEM((CB, *tile), F32),
            pltpu.VMEM((RB, *tile), F32),
            pltpu.VMEM((CB, *tile), F32),
            pltpu.VMEM((RB, 2 * SLOTS), BF16),
            pltpu.VMEM((CB, 2 * SLOTS), BF16),
            pltpu.VMEM((K * SLOTS, LANES), F32),
            pltpu.VMEM((K * SLOTS, LANES), F32),
            pltpu.VMEM((2, NC, K // 2, 2 * M, LANES), SUM_R),
            pltpu.VMEM((2, NR, K // 2, 2 * M, LANES), SUM_C),
            pltpu.VMEM((2, NC, K // 2, 2 * M, LANES), SUM_R),
            pltpu.VMEM((2, NR, K // 2, 2 * M, LANES), SUM_C),
            pltpu.VMEM((K * M, LANES), F32),
            pltpu.VMEM((2, M, *tile), F32),
            pltpu.VMEM((M, *tile), F32),
            pltpu.VMEM((3, 1, LANES), F32),
            pltpu.VMEM((3, NR * NC, 1, LANES), F32),
            pltpu.SemaphoreType.DMA((10,)),
            pltpu.SemaphoreType.DMA((18,)),
            pltpu.SemaphoreType.DMA((18,)),
        ],
        compiler_params=pltpu.CompilerParams(
            collective_id=0, has_side_effects=True, vmem_limit_bytes=67043328
        ),
        name="lanczos",
    )(start_block, blocks, block_rows, block_cols, counts.T)


def solution(mesh):
    assert mesh.shape["row"] == NR and mesh.shape["col"] == NC
    both = ("row", "col")
    return jax.shard_map(
        per_device,
        mesh=mesh,
        in_specs=(
            P(None, both),
            P("row", "col", None, None, None),
            P(None, "col", None),
            P(None, "col", None),
            P(),
        ),
        out_specs=(P(None, both), P()),
        check_vma=False,
    )
```

```python
import functools
import math

import jax
import jax.numpy as jnp
from jax import lax
from jax.experimental import pallas as pl
from jax.experimental.pallas import tpu as pltpu
from jax.sharding import PartitionSpec as P

F32 = jnp.float32
BF16 = jnp.bfloat16
MESH = pl.DeviceIdType.MESH

K = 8
LANES = 128
M = 8
SIDE = 4
NR, NC = 16, 8
RB, CB = NC * M, NR * M
SLOTS = 128
BATCH = 4
UNROLL = 16
SUM_C = BF16
SUM_R = BF16


def bcast(x):
    return jnp.broadcast_to(x, (K, LANES))


def kernel(
    x_hbm, blocks, rows_hbm, cols_hbm, counts_hbm,
    next_out, tri_out,
    bl, blt, x_in, rows_s, cols_s, counts_s, rows_v, cols_v, xb, yb, xr, xc, yr, yc, picks_r, picks_c, res_d, res_t,
    tot_r, tot_c, in_r, in_c, ykb, qown, wbuf, msg, ar, first, first_r, first_c,
    load_sem, send_sem, recv_sem,
):
    r = lax.axis_index("row")
    c = lax.axis_index("col")
    row_iota = lax.broadcasted_iota(jnp.int32, (K, LANES), 0)
    lane_iota = lax.broadcasted_iota(jnp.int32, (K, LANES), 1)

    def far(off):
        return -sum(min(d, SIDE - d) for d in off[:3]), off

    z0, x0 = r // SIDE, lax.rem(r, SIDE)
    y0, p0 = c // 2, lax.rem(c, 2)
    row_at = {
        (dz, dx): lax.rem(z0 + dz, SIDE) * SIDE + lax.rem(x0 + dx, SIDE) if dz + dx else r
        for dz in range(SIDE)
        for dx in range(SIDE)
    }
    col_at = {
        (dy, dp): lax.rem(y0 + dy, SIDE) * 2 + lax.rem(p0 + dp, 2) if dy + dp else c
        for dy in range(SIDE)
        for dp in range(2)
    }
    offsets = sorted(
        ((dz, dx, dy, dp) for dz, dx in row_at for dy, dp in col_at if dz + dx + dy + dp), key=far
    )
    others = [(row_at[o[:2]], col_at[o[2:]]) for o in offsets]
    row_peers = [row_at[o[:2]] for o in offsets if o[2:] == (0, 0)]
    col_peers = [col_at[o[2:]] for o in offsets if o[:2] == (0, 0)]

    barrier = pltpu.get_barrier_semaphore()
    for rr in row_peers:
        pl.semaphore_signal(barrier, inc=1, device_id=(rr, c), device_id_type=MESH)
    for cc in col_peers:
        pl.semaphore_signal(barrier, inc=1, device_id=(r, cc), device_id_type=MESH)

    parts = 4
    step = SLOTS // parts
    loads = [
        pltpu.make_async_copy(
            blocks.at[0, 0, pl.ds(i * step, step)], bl.at[pl.ds(i * step, step)], load_sem.at[i]
        )
        for i in range(parts)
    ]
    small = [
        pltpu.make_async_copy(src, dst, load_sem.at[parts + i])
        for i, (src, dst) in enumerate(
            [
                (x_hbm, x_in),
                (rows_hbm.at[r], rows_s),
                (cols_hbm.at[r], cols_s),
                (counts_hbm, counts_s),
                (rows_hbm.at[r], rows_v),
                (cols_hbm.at[r], cols_v),
            ]
        )
    ]
    for load in small + loads:
        load.start()

    def send(src, dst, sems, dev):
        pltpu.make_async_remote_copy(
            src_ref=src, dst_ref=dst, send_sem=send_sem.at[sems], recv_sem=recv_sem.at[sems],
            device_id=dev, device_id_type=MESH,
        ).start()

    def wait_bytes(ref, sem):
        pltpu.make_async_copy(ref, ref, sem).wait()

    def gram(a_ref, b_ref, lane0, tile):
        for j in range(K):
            acc = None
            for b in range(M):
                term = a_ref[b] * b_ref[b, pl.ds(j, 1), :]
                acc = term if acc is None else acc + term
            col = jnp.sum(acc, axis=1, keepdims=True)
            tile = jnp.where(lane_iota == 2 * K * row_iota + (lane0 + j), bcast(col), tile)
        return tile

    def tree(terms):
        while len(terms) > 1:
            terms = [p + q for p, q in zip(terms[::2], terms[1::2])]
        return terms[0]

    def first_reduce_start(tile):
        first[0] = jnp.sum(tile, axis=0, keepdims=True)
        for rr in row_peers:
            send(first.at[0], first_r.at[r], 18, (rr, c))

    def first_reduce_finish():
        wait_bytes(first_r.at[pl.ds(0, NR - 1)], recv_sem.at[18])
        first_r[r] = first[0]
        first[1] = tree([first_r[i] for i in range(NR)])
        for cc in col_peers:
            send(first.at[1], first_c.at[c], 19, (r, cc))
        wait_bytes(first_c.at[pl.ds(0, NC - 1)], recv_sem.at[19])
        first_c[c] = first[1]
        return bcast(tree([first_c[i] for i in range(NC)]))

    def reduce_start(n, tile):
        msg[n] = jnp.sum(tile, axis=0, keepdims=True)
        for dev in others:
            send(msg.at[n], ar.at[n, r * NC + c], 6 * n, dev)

    def reduce_finish(n):
        wait_bytes(ar.at[n, pl.ds(0, NR * NC - 1)], recv_sem.at[6 * n])
        ar[n, r * NC + c] = msg[n]
        sums = [ar[n, i] for i in range(8)]
        for i in range(8, NR * NC):
            sums[i % 8] = sums[i % 8] + ar[n, i]
        return bcast(tree(sums))

    def picked(total, lanes):
        return bcast(jnp.sum(jnp.where(lane_iota == lanes, total, 0.0), axis=1, keepdims=True))

    def columns(total, lane0):
        return [picked(total, 2 * K * row_iota + (lane0 + j)) for j in range(K)]

    def rows_of(total):
        return [picked(total, row_iota + 2 * K * j) for j in range(K)]

    def factor(gcols):
        g = list(gcols)
        d = [jnp.where(row_iota == m, 1.0, 0.0).astype(F32) for m in range(K)]
        unit = []
        diag = g[0]
        for j in range(K):
            inv = 1.0 / g[j][j : j + 1, :]
            f = jnp.where(row_iota > j, g[j] * inv, 0.0)
            unit.append(f + jnp.where(row_iota == j, 1.0, 0.0))
            if j:
                diag = jnp.where(row_iota == j, g[j], diag)
            for m in range(j + 1, K):
                g[m] = g[m] - f * g[m][j : j + 1, :]
            for m in range(j + 1):
                d[m] = d[m] - f * d[m][j : j + 1, :]
        root = jnp.sqrt(diag)
        rs = 1.0 / root
        inverse = [v * rs for v in d]
        upper = [jnp.where(row_iota <= m, g[m], 0.0) * rs for m in range(K)]
        lower = [unit[j] * root[j : j + 1, :] for j in range(K)]
        return inverse, upper, lower

    def matmul_cols(left, right):
        out = []
        for m in range(K):
            acc = left[0] * right[m][0:1, :]
            for p in range(1, K):
                acc = acc + left[p] * right[m][p : p + 1, :]
            out.append(acc)
        return out

    def apply(cols, ref, i):
        acc = cols[0] * ref[i, pl.ds(0, 1), :]
        for j in range(1, K):
            acc = acc + cols[j] * ref[i, pl.ds(j, 1), :]
        return acc

    def gather_start(src, seg_r, seg_c, n):
        for cc in col_peers:
            send(src, seg_r.at[pl.ds(M * c, M)], 6 * n + 3, (r, cc))
        for rr in row_peers:
            send(src, seg_c.at[pl.ds(M * r, M)], 6 * n + 2, (rr, c))
        for b in range(M):
            seg_c[M * r + b] = src[b]
            seg_r[M * c + b] = src[b]

    def gather_wait_col(seg_r, n):
        wait_bytes(seg_r.at[pl.ds(0, (NC - 1) * M)], recv_sem.at[6 * n + 3])

    def gather_wait_row(seg_c, n):
        wait_bytes(seg_c.at[pl.ds(0, (NR - 1) * M)], recv_sem.at[6 * n + 2])

    zero = jnp.zeros((K, LANES), F32)

    def cat(a, b, axis):
        return jnp.concatenate([a, b], axis=axis)

    def product(vec, ids, mats, res):
        def body(q, carry):
            base = BATCH * q
            b = [mats[base + i] for i in range(BATCH)]
            tile = cat(cat(b[0], b[1], 0), cat(b[2], b[3], 0), 1)
            x = [vec[ids[0, base + i]] for i in range(BATCH)]
            lhs = jnp.concatenate(
                [cat(zero, x[i], 1) if i % 2 else cat(x[i], zero, 1) for i in range(BATCH)], axis=0
            ).astype(BF16)
            out = jnp.dot(lhs, tile, preferred_element_type=F32)
            for i in range(BATCH):
                half = LANES * (i // 2)
                res[pl.ds(base + i, K, stride=SLOTS), :] = out[K * i : K * i + K, half : half + LANES]
            return carry

        lax.fori_loop(0, SLOTS // BATCH, body, 0, unroll=UNROLL)

    def scatter(pick, res, put):
        for kk in range(K // 2):
            full = cat(
                res[pl.ds(2 * kk * SLOTS, SLOTS), :], res[pl.ds((2 * kk + 1) * SLOTS, SLOTS), :], 1
            )
            hi = full.astype(BF16)
            lo = (full - hi.astype(F32)).astype(BF16)
            put(kk, jnp.dot(pick[...], cat(hi, lo, 0), preferred_element_type=F32))

    def exchange_cols(n):
        def put(kk, out):
            for i in range(NR):
                rows = out[M * i : M * i + M]
                tot_c[n, i, kk] = cat(rows[:, :LANES], rows[:, LANES:], 0).astype(tot_c.dtype)

        scatter(picks_c, res_t, put)
        for rr in row_peers:
            send(tot_c.at[n, rr], in_c.at[n, r], 6 * n + 4, (rr, c))
        in_c[n, r] = tot_c[n, r]

    def exchange_rows(n):
        def put(kk, out):
            for i in range(NC):
                rows = out[M * i : M * i + M]
                tot_r[n, i, kk] = cat(rows[:, :LANES], rows[:, LANES:], 0).astype(tot_r.dtype)

        scatter(picks_r, res_d, put)
        for cc in col_peers:
            send(tot_r.at[n, cc], in_r.at[n, c], 6 * n + 5, (r, cc))
        in_r[n, c] = tot_r[n, c]

    def exchange_finish(n, out_ref):
        wait_bytes(in_r.at[n, pl.ds(0, NC - 1)], recv_sem.at[6 * n + 5])
        for kk in range(K // 2):
            total = in_r[n, 0, kk].astype(F32)
            for i in range(1, NC):
                total = total + in_r[n, i, kk].astype(F32)
            ykb[pl.ds(2 * M * kk, 2 * M), :] = total
        wait_bytes(in_c.at[n, pl.ds(0, NR - 1)], recv_sem.at[6 * n + 4])
        for kk in range(K // 2):
            total = ykb[pl.ds(2 * M * kk, 2 * M), :]
            for i in range(NR):
                total = total + in_c[n, i, kk].astype(F32)
            ykb[pl.ds(2 * M * kk, 2 * M), :] = total
        for b in range(M):
            out_ref[b] = ykb[pl.ds(b, K, stride=M), :]

    def sweep(count, step, update):
        def body(i, carry):
            for u in range(step):
                update(step * i + u)
            return carry

        lax.fori_loop(0, count // step, body, 0)

    for load in small:
        load.wait()
    for b in range(M):
        xb[b] = x_in[:, pl.ds(LANES * b, LANES)]
    start_tile = gram(xb, xb, 0, zero)

    giota = lax.broadcasted_iota(jnp.int32, (1, SLOTS), 1)
    row_ids = rows_v[...]
    col_ids = cols_v[...]
    valid = giota < counts_s[c, r]
    global_row = r * RB + row_ids
    global_col = ((col_ids // M) * NC + c) * M + lax.rem(col_ids, M)
    mirror = jnp.logical_and(valid, global_row != global_col)
    want_r = jnp.where(valid, row_ids, -1)
    want_c = jnp.where(mirror, col_ids, -1)
    one_r = jnp.where(lax.broadcasted_iota(jnp.int32, (RB, SLOTS), 0) == want_r, 1.0, 0.0)
    one_c = jnp.where(lax.broadcasted_iota(jnp.int32, (CB, SLOTS), 0) == want_c, 1.0, 0.0)
    one_r = one_r.astype(BF16)
    one_c = one_c.astype(BF16)
    picks_r[...] = cat(one_r, one_r, 1)
    picks_c[...] = cat(one_c, one_c, 1)

    pl.semaphore_wait(barrier, NR + NC - 2)

    first_reduce_start(start_tile)
    gather_start(xb, xr, xc, 0)
    for load in loads:
        load.wait()

    def turn(i, carry):
        for u in range(8):
            blt[8 * i + u] = bl[8 * i + u].T
        return carry

    lax.fori_loop(0, SLOTS // 8, turn, 0)
    inverse, _, _ = factor(columns(first_reduce_finish(), 0))

    def normalise(seg, t):
        seg[t] = apply(inverse, seg, t)

    gather_wait_col(xr, 0)
    sweep(RB, 8, functools.partial(normalise, xr))
    product(xr, rows_s, bl, res_t)
    exchange_cols(0)
    gather_wait_row(xc, 0)
    sweep(CB, 8, functools.partial(normalise, xc))
    product(xc, cols_s, blt, res_d)
    exchange_rows(0)
    for b in range(M):
        qown[0, b] = xr[M * c + b]
    exchange_finish(0, yb)

    tile = gram(yb, qown.at[0], 0, zero)
    tile = gram(yb, yb, K, tile)
    reduce_start(1, tile)
    gather_start(yb, yr, yc, 1)
    total = reduce_finish(1)
    at_cols = columns(total, 0)
    s_cols = columns(total, K)
    a1_cols = rows_of(total)
    ata = matmul_cols(at_cols, a1_cols)
    inverse, upper1, lower1 = factor([s - t for s, t in zip(s_cols, ata)])
    back = matmul_cols(inverse, at_cols)

    def advance(seg, old, t):
        seg[t] = apply(inverse, seg, t) - apply(back, old, t)

    gather_wait_col(yr, 1)
    sweep(RB, 4, functools.partial(advance, yr, xr))
    product(yr, rows_s, bl, res_t)
    exchange_cols(1)
    gather_wait_row(yc, 1)
    sweep(CB, 4, functools.partial(advance, yc, xc))
    product(yc, cols_s, blt, res_d)
    exchange_rows(1)
    for b in range(M):
        qown[1, b] = yr[M * c + b]
    top = zero
    for j in range(K):
        top = jnp.where(lane_iota == j, a1_cols[j], top)
        top = jnp.where(lane_iota == K + j, lower1[j], top)
    tri_out[pl.ds(0, K), :] = top[:, : 2 * K]
    exchange_finish(1, wbuf)
    for b in range(M):
        wbuf[b] = wbuf[b] - apply(upper1, qown.at[0], b)
    tile = gram(wbuf, qown.at[1], 0, zero)
    tile = gram(wbuf, wbuf, K, tile)
    reduce_start(2, tile)

    wait_bytes(first_r.at[pl.ds(0, NR - 1)], send_sem.at[18])
    wait_bytes(first_c.at[pl.ds(0, NC - 1)], send_sem.at[19])
    wait_bytes(ar.at[1, pl.ds(0, NR * NC - 1)], send_sem.at[6])
    for n in range(2):
        wait_bytes(xc.at[pl.ds(0, (NR - 1) * M)], send_sem.at[6 * n + 2])
        wait_bytes(xr.at[pl.ds(0, (NC - 1) * M)], send_sem.at[6 * n + 3])
        wait_bytes(in_c.at[n, pl.ds(0, NR - 1)], send_sem.at[6 * n + 4])
        wait_bytes(in_r.at[n, pl.ds(0, NC - 1)], send_sem.at[6 * n + 5])

    total = reduce_finish(2)
    at_cols = columns(total, 0)
    s_cols = columns(total, K)
    a2_cols = rows_of(total)
    ata = matmul_cols(at_cols, a2_cols)
    inverse, _, _ = factor([s - t for s, t in zip(s_cols, ata)])
    back = matmul_cols(inverse, at_cols)
    order_root = math.sqrt(NR * NC * M * LANES)
    for b in range(M):
        value = apply(inverse, wbuf, b) - apply(back, qown.at[1], b)
        next_out[:, pl.ds(LANES * b, LANES)] = value * order_root
    low = zero
    for j in range(K):
        low = jnp.where(lane_iota == j, upper1[j], low)
        low = jnp.where(lane_iota == K + j, a2_cols[j], low)
    tri_out[pl.ds(K, K), :] = low[:, : 2 * K]
    wait_bytes(ar.at[2, pl.ds(0, NR * NC - 1)], send_sem.at[12])


def per_device(start_block, blocks, block_rows, block_cols, counts):
    args = (start_block, blocks, block_rows, block_cols, counts.T)
    vmem = pl.BlockSpec(memory_space=pltpu.VMEM)
    hbm = pl.BlockSpec(memory_space=pltpu.HBM)
    tile = (K, LANES)
    return pl.pallas_call(
        kernel,
        out_shape=(
            jax.ShapeDtypeStruct((K, M * LANES), F32),
            jax.ShapeDtypeStruct((2 * K, 2 * K), F32),
        ),
        in_specs=[hbm] * 5,
        out_specs=(vmem, vmem),
        scratch_shapes=[
            pltpu.VMEM((SLOTS, LANES, LANES), BF16),
            pltpu.VMEM((SLOTS, LANES, LANES), BF16),
            pltpu.VMEM((K, M * LANES), F32),
            pltpu.SMEM((1, SLOTS), jnp.int32),
            pltpu.SMEM((1, SLOTS), jnp.int32),
            pltpu.SMEM((NC, NR), jnp.int32),
            pltpu.VMEM((1, SLOTS), jnp.int32),
            pltpu.VMEM((1, SLOTS), jnp.int32),
            pltpu.VMEM((M, *tile), F32),
            pltpu.VMEM((M, *tile), F32),
            pltpu.VMEM((RB, *tile), F32),
            pltpu.VMEM((CB, *tile), F32),
            pltpu.VMEM((RB, *tile), F32),
            pltpu.VMEM((CB, *tile), F32),
            pltpu.VMEM((RB, 2 * SLOTS), BF16),
            pltpu.VMEM((CB, 2 * SLOTS), BF16),
            pltpu.VMEM((K * SLOTS, LANES), F32),
            pltpu.VMEM((K * SLOTS, LANES), F32),
            pltpu.VMEM((2, NC, K // 2, 2 * M, LANES), SUM_R),
            pltpu.VMEM((2, NR, K // 2, 2 * M, LANES), SUM_C),
            pltpu.VMEM((2, NC, K // 2, 2 * M, LANES), SUM_R),
            pltpu.VMEM((2, NR, K // 2, 2 * M, LANES), SUM_C),
            pltpu.VMEM((K * M, LANES), F32),
            pltpu.VMEM((2, M, *tile), F32),
            pltpu.VMEM((M, *tile), F32),
            pltpu.VMEM((3, 1, LANES), F32),
            pltpu.VMEM((3, NR * NC, 1, LANES), F32),
            pltpu.VMEM((2, 1, LANES), F32),
            pltpu.VMEM((NR, 1, LANES), F32),
            pltpu.VMEM((NC, 1, LANES), F32),
            pltpu.SemaphoreType.DMA((10,)),
            pltpu.SemaphoreType.DMA((20,)),
            pltpu.SemaphoreType.DMA((20,)),
        ],
        compiler_params=pltpu.CompilerParams(
            collective_id=0, has_side_effects=True, vmem_limit_bytes=48 * 1024 * 1024
        ),
        name="lanczos",
    )(*[pltpu.with_memory_space_constraint(v, pltpu.HBM) for v in args])


def solution(mesh):
    assert mesh.shape["row"] == NR and mesh.shape["col"] == NC
    both = ("row", "col")
    return jax.shard_map(
        per_device,
        mesh=mesh,
        in_specs=(
            P(None, both),
            P("row", "col", None, None, None),
            P(None, "col", None),
            P(None, "col", None),
            P(),
        ),
        out_specs=(P(None, both), P()),
        check_vma=False,
    )
```

```python
import math

import jax
import jax.numpy as jnp
from jax import lax
from jax.experimental import pallas as pl
from jax.experimental.pallas import tpu as pltpu
from jax.sharding import PartitionSpec as P

F32 = jnp.float32
BF16 = jnp.bfloat16
MESH = pl.DeviceIdType.MESH

K = 8
LANES = 128
M = 8
SIDE = 4
NR, NC = 16, 8
RB, CB = NC * M, NR * M
SLOTS = 128
BATCH = 4
UNROLL = 16
I16 = jnp.int16
TOP = 32700.0
TINY = 1e-30


def bcast(x):
    return jnp.broadcast_to(x, (K, LANES))


def kernel(
    x_hbm, blocks, rows_hbm, cols_hbm, counts_hbm,
    next_out, tri_out,
    bl, blt, x_in, rows_s, cols_s, counts_s, rows_v, cols_v, xb, yb, yraw, zb, wb, q1, q2,
    own_q, own_s, seg_qr, seg_sr, seg_qc, seg_sc, spread, vr, vc, picks_r, picks_c, most, res_d, res_t,
    tot_r, tot_c, sum_sr, sum_sc, in_r, in_c, in_sr, in_sc, ykb, msg, ar, first, first_r, first_c,
    load_sem, send_sem, recv_sem,
):
    r = lax.axis_index("row")
    c = lax.axis_index("col")
    row_iota = lax.broadcasted_iota(jnp.int32, (K, LANES), 0)
    lane_iota = lax.broadcasted_iota(jnp.int32, (K, LANES), 1)

    def far(off):
        return -sum(min(d, SIDE - d) for d in off[:3]), off

    z0, x0 = r // SIDE, lax.rem(r, SIDE)
    y0, p0 = c // 2, lax.rem(c, 2)
    row_at = {
        (dz, dx): lax.rem(z0 + dz, SIDE) * SIDE + lax.rem(x0 + dx, SIDE) if dz + dx else r
        for dz in range(SIDE)
        for dx in range(SIDE)
    }
    col_at = {
        (dy, dp): lax.rem(y0 + dy, SIDE) * 2 + lax.rem(p0 + dp, 2) if dy + dp else c
        for dy in range(SIDE)
        for dp in range(2)
    }
    offsets = sorted(
        ((dz, dx, dy, dp) for dz, dx in row_at for dy, dp in col_at if dz + dx + dy + dp), key=far
    )
    others = [(row_at[o[:2]], col_at[o[2:]]) for o in offsets]
    row_peers = [row_at[o[:2]] for o in offsets if o[2:] == (0, 0)]
    col_peers = [col_at[o[2:]] for o in offsets if o[:2] == (0, 0)]

    barrier = pltpu.get_barrier_semaphore()
    for rr in row_peers:
        pl.semaphore_signal(barrier, inc=1, device_id=(rr, c), device_id_type=MESH)
    for cc in col_peers:
        pl.semaphore_signal(barrier, inc=1, device_id=(r, cc), device_id_type=MESH)

    parts = 4
    step = SLOTS // parts
    loads = [
        pltpu.make_async_copy(
            blocks.at[0, 0, pl.ds(i * step, step)], bl.at[pl.ds(i * step, step)], load_sem.at[i]
        )
        for i in range(parts)
    ]
    small = [
        pltpu.make_async_copy(src, dst, load_sem.at[parts + i])
        for i, (src, dst) in enumerate(
            [
                (x_hbm, x_in),
                (rows_hbm.at[r], rows_s),
                (cols_hbm.at[r], cols_s),
                (counts_hbm, counts_s),
                (rows_hbm.at[r], rows_v),
                (cols_hbm.at[r], cols_v),
            ]
        )
    ]
    for load in small + loads:
        load.start()

    def send(src, dst, sems, dev):
        pltpu.make_async_remote_copy(
            src_ref=src, dst_ref=dst, send_sem=send_sem.at[sems], recv_sem=recv_sem.at[sems],
            device_id=dev, device_id_type=MESH,
        ).start()

    def wait_bytes(ref, sem):
        pltpu.make_async_copy(ref, ref, sem).wait()

    def gram(a_ref, b_ref, lane0, tile):
        for j in range(K):
            acc = None
            for b in range(M):
                term = a_ref[b] * b_ref[b, pl.ds(j, 1), :]
                acc = term if acc is None else acc + term
            col = jnp.sum(acc, axis=1, keepdims=True)
            tile = jnp.where(lane_iota == 2 * K * row_iota + (lane0 + j), bcast(col), tile)
        return tile

    def tree(terms):
        while len(terms) > 1:
            terms = [p + q for p, q in zip(terms[::2], terms[1::2])]
        return terms[0]

    def first_reduce_start(tile):
        first[0] = jnp.sum(tile, axis=0, keepdims=True)
        for rr in row_peers:
            send(first.at[0], first_r.at[r], 18, (rr, c))

    def first_reduce_turn():
        wait_bytes(first_r.at[pl.ds(0, NR - 1)], recv_sem.at[18])
        first_r[r] = first[0]
        first[1] = tree([first_r[i] for i in range(NR)])
        for cc in col_peers:
            send(first.at[1], first_c.at[c], 19, (r, cc))

    def first_reduce_finish():
        wait_bytes(first_c.at[pl.ds(0, NC - 1)], recv_sem.at[19])
        first_c[c] = first[1]
        return bcast(tree([first_c[i] for i in range(NC)]))

    def reduce_start(n, tile):
        msg[n] = jnp.sum(tile, axis=0, keepdims=True)
        for dev in others:
            send(msg.at[n], ar.at[n, r * NC + c], 16 + n, dev)

    def reduce_finish(n):
        wait_bytes(ar.at[n, pl.ds(0, NR * NC - 1)], recv_sem.at[16 + n])
        ar[n, r * NC + c] = msg[n]
        sums = [ar[n, i] for i in range(8)]
        for i in range(8, NR * NC):
            sums[i % 8] = sums[i % 8] + ar[n, i]
        return bcast(tree(sums))

    def picked(total, lanes):
        return bcast(jnp.sum(jnp.where(lane_iota == lanes, total, 0.0), axis=1, keepdims=True))

    def columns(total, lane0):
        return [picked(total, 2 * K * row_iota + (lane0 + j)) for j in range(K)]

    def rows_of(total):
        return [picked(total, row_iota + 2 * K * j) for j in range(K)]

    def factor(gcols):
        g = list(gcols)
        d = [jnp.where(row_iota == m, 1.0, 0.0).astype(F32) for m in range(K)]
        unit = []
        diag = g[0]
        for j in range(K):
            inv = 1.0 / g[j][j : j + 1, :]
            f = jnp.where(row_iota > j, g[j] * inv, 0.0)
            unit.append(f + jnp.where(row_iota == j, 1.0, 0.0))
            if j:
                diag = jnp.where(row_iota == j, g[j], diag)
            for m in range(j + 1, K):
                g[m] = g[m] - f * g[m][j : j + 1, :]
            for m in range(j + 1):
                d[m] = d[m] - f * d[m][j : j + 1, :]
        root = jnp.sqrt(diag)
        rs = 1.0 / root
        inverse = [v * rs for v in d]
        upper = [jnp.where(row_iota <= m, g[m], 0.0) * rs for m in range(K)]
        lower = [unit[j] * root[j : j + 1, :] for j in range(K)]
        return inverse, upper, lower

    def matmul_cols(left, right):
        out = []
        for m in range(K):
            acc = left[0] * right[m][0:1, :]
            for p in range(1, K):
                acc = acc + left[p] * right[m][p : p + 1, :]
            out.append(acc)
        return out

    def apply(cols, ref, i):
        acc = cols[0] * ref[i, pl.ds(0, 1), :]
        for j in range(1, K):
            acc = acc + cols[j] * ref[i, pl.ds(j, 1), :]
        return acc

    zero = jnp.zeros((K, LANES), F32)
    zero_pair = jnp.zeros((2 * K, LANES), BF16)

    def cat(a, b, axis):
        return jnp.concatenate([a, b], axis=axis)

    def fixed(value):
        return jnp.round(value).astype(jnp.int32).astype(I16)

    def scales(largest):
        m = jnp.maximum(bcast(jnp.max(largest, axis=1, keepdims=True)), TINY)
        return TOP / m, m * (1.0 / TOP)

    def to_row(scale):
        return jnp.sum(jnp.where(lane_iota == row_iota, scale, 0.0), axis=0, keepdims=True)

    def unpack_scales(row_ref, col_ref):
        for i in range(NC):
            spread[i] = picked(bcast(row_ref[i]), row_iota)
        for i in range(NR):
            spread[NC + i] = picked(bcast(col_ref[i]), row_iota)

    def quantise(src, n):
        largest = jnp.abs(src[0])
        for b in range(1, M):
            largest = jnp.maximum(largest, jnp.abs(src[b]))
        inv, scale = scales(largest)
        for bb in range(M // 2):
            own_q[n, bb] = fixed(cat(src[2 * bb] * inv, src[2 * bb + 1] * inv, 0))
        own_s[n] = to_row(scale)

    def gather_start(n):
        for cc in col_peers:
            send(own_s.at[n], seg_sr.at[n, c], 8 * n + 0, (r, cc))
            send(own_q.at[n], seg_qr.at[n, c], 8 * n + 1, (r, cc))
        for rr in row_peers:
            send(own_s.at[n], seg_sc.at[n, r], 8 * n + 2, (rr, c))
            send(own_q.at[n], seg_qc.at[n, r], 8 * n + 3, (rr, c))
        seg_sr[n, c] = own_s[n]
        seg_qr[n, c] = own_q[n]
        seg_sc[n, r] = own_s[n]
        seg_qc[n, r] = own_q[n]

    def split(pieces, quant, scale_row, vec, group):
        def body(i, carry):
            for u in range(group):
                p = group * i + u
                scale = picked(bcast(scale_row[p]), row_iota)
                for bb in range(M // 2):
                    both = quant[p, bb].astype(jnp.int32).astype(F32)
                    for h in range(2):
                        value = both[K * h : K * h + K] * scale
                        high = value.astype(BF16).astype(F32)
                        vec[M * p + 2 * bb + h] = cat(value, value - high, 0).astype(BF16)
            return carry

        lax.fori_loop(0, pieces // group, body, 0)

    def gather_row_segment(n):
        wait_bytes(seg_sr.at[n, pl.ds(0, NC - 1)], recv_sem.at[8 * n + 0])
        wait_bytes(seg_qr.at[n, pl.ds(0, NC - 1)], recv_sem.at[8 * n + 1])
        split(NC, seg_qr.at[n], seg_sr.at[n], vr, 4)

    def gather_col_segment(n):
        wait_bytes(seg_sc.at[n, pl.ds(0, NR - 1)], recv_sem.at[8 * n + 2])
        wait_bytes(seg_qc.at[n, pl.ds(0, NR - 1)], recv_sem.at[8 * n + 3])
        split(NR, seg_qc.at[n], seg_sc.at[n], vc, 4)

    def product(vec, ids, mats, res):
        count = counts_s[c, r]

        def body(q, largest):
            base = BATCH * q
            b = [mats[base + i] for i in range(BATCH)]
            tile = cat(cat(b[0], b[1], 0), cat(b[2], b[3], 0), 1)
            x = [vec[ids[0, base + i]] for i in range(BATCH)]
            lhs = jnp.concatenate(
                [
                    cat(zero_pair, x[i], 1) if i % 2 else cat(x[i], zero_pair, 1)
                    for i in range(BATCH)
                ],
                axis=0,
            )
            out = jnp.dot(lhs, tile, preferred_element_type=F32)
            for i in range(BATCH):
                half = LANES * (i // 2)
                part = out[2 * K * i : 2 * K * i + 2 * K, half : half + LANES]
                part = part[:K] + part[K:]
                res[pl.ds(base + i, K, stride=SLOTS), :] = part
                largest = jnp.maximum(largest, jnp.where(base + i < count, jnp.abs(part), 0.0))
            return largest

        return lax.fori_loop(0, SLOTS // BATCH, body, zero, unroll=UNROLL)

    def scatter(pick, res, largest, bound, tot, pieces):
        inv, scale = scales(largest * bound)
        for kk in range(K // 2):
            full = cat(
                res[pl.ds(2 * kk * SLOTS, SLOTS), :], res[pl.ds((2 * kk + 1) * SLOTS, SLOTS), :], 1
            )
            hi = full.astype(BF16)
            lo = (full - hi.astype(F32)).astype(BF16)
            out = jnp.dot(pick[...], cat(hi, lo, 0), preferred_element_type=F32)
            even = bcast(inv[2 * kk : 2 * kk + 1, :])
            odd = bcast(inv[2 * kk + 1 : 2 * kk + 2, :])
            for i in range(pieces):
                rows = out[M * i : M * i + M]
                tot[i, kk] = fixed(cat(rows[:, :LANES] * even, rows[:, LANES:] * odd, 0))
        return to_row(scale)

    def exchange_cols(n, largest):
        sum_sc[n] = scatter(picks_c, res_t, largest, most[1], tot_c.at[n], NR)
        for rr in row_peers:
            send(sum_sc.at[n], in_sc.at[n, r], 8 * n + 4, (rr, c))
            send(tot_c.at[n, rr], in_c.at[n, r], 8 * n + 5, (rr, c))
        in_sc[n, r] = sum_sc[n]
        in_c[n, r] = tot_c[n, r]

    def exchange_rows(n, largest):
        sum_sr[n] = scatter(picks_r, res_d, largest, most[0], tot_r.at[n], NC)
        for cc in col_peers:
            send(sum_sr.at[n], in_sr.at[n, c], 8 * n + 6, (r, cc))
            send(tot_r.at[n, cc], in_r.at[n, c], 8 * n + 7, (r, cc))
        in_sr[n, c] = sum_sr[n]
        in_r[n, c] = tot_r[n, c]

    def exchange_finish(n, out_ref):
        wait_bytes(in_sr.at[n, pl.ds(0, NC - 1)], recv_sem.at[8 * n + 6])
        wait_bytes(in_sc.at[n, pl.ds(0, NR - 1)], recv_sem.at[8 * n + 4])
        unpack_scales(in_sr.at[n], in_sc.at[n])

        def term(ref, i, kk, at):
            even = bcast(spread[at + i, pl.ds(2 * kk, 1), :])
            odd = bcast(spread[at + i, pl.ds(2 * kk + 1, 1), :])
            return ref[n, i, kk].astype(jnp.int32).astype(F32) * cat(even, odd, 0)

        wait_bytes(in_r.at[n, pl.ds(0, NC - 1)], recv_sem.at[8 * n + 7])
        wait_bytes(in_c.at[n, pl.ds(0, NR - 1)], recv_sem.at[8 * n + 5])
        for kk in range(K // 2):
            terms = [term(in_r, i, kk, 0) for i in range(NC)]
            total = tree(terms)
            terms = [term(in_c, i, kk, NC) for i in range(NR)]
            ykb[pl.ds(2 * M * kk, 2 * M), :] = total + tree(terms)
        for b in range(M):
            out_ref[b] = ykb[pl.ds(b, K, stride=M), :]

    for load in small:
        load.wait()
    for b in range(M):
        xb[b] = x_in[:, pl.ds(LANES * b, LANES)]
    start_tile = gram(xb, xb, 0, zero)
    quantise(xb, 0)

    giota = lax.broadcasted_iota(jnp.int32, (1, SLOTS), 1)
    row_ids = rows_v[...]
    col_ids = cols_v[...]
    valid = giota < counts_s[c, r]
    global_row = r * RB + row_ids
    global_col = ((col_ids // M) * NC + c) * M + lax.rem(col_ids, M)
    mirror = jnp.logical_and(valid, global_row != global_col)
    want_r = jnp.where(valid, row_ids, -1)
    want_c = jnp.where(mirror, col_ids, -1)
    one_r = jnp.where(lax.broadcasted_iota(jnp.int32, (RB, SLOTS), 0) == want_r, 1.0, 0.0)
    one_c = jnp.where(lax.broadcasted_iota(jnp.int32, (CB, SLOTS), 0) == want_c, 1.0, 0.0)
    for i, one in enumerate((one_r, one_c)):
        most[i] = bcast(jnp.max(jnp.sum(one, axis=1, keepdims=True), axis=0, keepdims=True))
    one_r = one_r.astype(BF16)
    one_c = one_c.astype(BF16)
    picks_r[...] = cat(one_r, one_r, 1)
    picks_c[...] = cat(one_c, one_c, 1)

    pl.semaphore_wait(barrier, NR + NC - 2)

    first_reduce_start(start_tile)
    gather_start(0)
    for load in loads:
        load.wait()

    def turn(i, carry):
        for u in range(8):
            blt[8 * i + u] = bl[8 * i + u].T
        return carry

    lax.fori_loop(0, SLOTS // 8, turn, 0)

    gather_row_segment(0)
    largest = product(vr, rows_s, bl, res_t)
    exchange_cols(0, largest)
    first_reduce_turn()
    gather_col_segment(0)
    largest = product(vc, cols_s, blt, res_d)
    exchange_rows(0, largest)
    inverse, _, _ = factor(columns(first_reduce_finish(), 0))
    for b in range(M):
        q1[b] = apply(inverse, xb, b)
    exchange_finish(0, yraw)
    for b in range(M):
        yb[b] = apply(inverse, yraw, b)

    quantise(yb, 1)
    gather_start(1)
    tile = gram(yb, q1, 0, zero)
    tile = gram(yb, yb, K, tile)
    reduce_start(0, tile)
    gather_row_segment(1)
    largest = product(vr, rows_s, bl, res_t)
    exchange_cols(1, largest)
    gather_col_segment(1)
    largest = product(vc, cols_s, blt, res_d)
    exchange_rows(1, largest)
    total = reduce_finish(0)
    at_cols = columns(total, 0)
    s_cols = columns(total, K)
    a1_cols = rows_of(total)
    ata = matmul_cols(at_cols, a1_cols)
    inverse, upper1, lower1 = factor([s - t for s, t in zip(s_cols, ata)])
    back = matmul_cols(inverse, at_cols)
    for b in range(M):
        q2[b] = apply(inverse, yb, b) - apply(back, q1, b)
        wb[b] = apply(back, yb, b) + apply(upper1, q1, b)
    top = zero
    for j in range(K):
        top = jnp.where(lane_iota == j, a1_cols[j], top)
        top = jnp.where(lane_iota == K + j, lower1[j], top)
    tri_out[pl.ds(0, K), :] = top[:, : 2 * K]
    exchange_finish(1, zb)
    for b in range(M):
        wb[b] = apply(inverse, zb, b) - wb[b]
    tile = gram(wb, q2, 0, zero)
    tile = gram(wb, wb, K, tile)
    reduce_start(1, tile)

    wait_bytes(first_r.at[pl.ds(0, NR - 1)], send_sem.at[18])
    wait_bytes(first_c.at[pl.ds(0, NC - 1)], send_sem.at[19])
    wait_bytes(ar.at[0, pl.ds(0, NR * NC - 1)], send_sem.at[16])
    for n in range(2):
        for i, (ref, count) in enumerate(
            [
                (seg_sr, NC), (seg_qr, NC), (seg_sc, NR), (seg_qc, NR),
                (in_sc, NR), (in_c, NR), (in_sr, NC), (in_r, NC),
            ]
        ):
            wait_bytes(ref.at[n, pl.ds(0, count - 1)], send_sem.at[8 * n + i])

    total = reduce_finish(1)
    at_cols = columns(total, 0)
    s_cols = columns(total, K)
    a2_cols = rows_of(total)
    ata = matmul_cols(at_cols, a2_cols)
    inverse, _, _ = factor([s - t for s, t in zip(s_cols, ata)])
    back = matmul_cols(inverse, at_cols)
    order_root = math.sqrt(NR * NC * M * LANES)
    for b in range(M):
        value = apply(inverse, wb, b) - apply(back, q2, b)
        next_out[:, pl.ds(LANES * b, LANES)] = value * order_root
    low = zero
    for j in range(K):
        low = jnp.where(lane_iota == j, upper1[j], low)
        low = jnp.where(lane_iota == K + j, a2_cols[j], low)
    tri_out[pl.ds(K, K), :] = low[:, : 2 * K]
    wait_bytes(ar.at[1, pl.ds(0, NR * NC - 1)], send_sem.at[17])


def per_device(start_block, blocks, block_rows, block_cols, counts):
    args = (start_block, blocks, block_rows, block_cols, counts.T)
    vmem = pl.BlockSpec(memory_space=pltpu.VMEM)
    hbm = pl.BlockSpec(memory_space=pltpu.HBM)
    tile = (K, LANES)
    pair = (2 * K, LANES)
    return pl.pallas_call(
        kernel,
        out_shape=(
            jax.ShapeDtypeStruct((K, M * LANES), F32),
            jax.ShapeDtypeStruct((2 * K, 2 * K), F32),
        ),
        in_specs=[hbm] * 5,
        out_specs=(vmem, vmem),
        scratch_shapes=[
            pltpu.VMEM((SLOTS, LANES, LANES), BF16),
            pltpu.VMEM((SLOTS, LANES, LANES), BF16),
            pltpu.VMEM((K, M * LANES), F32),
            pltpu.SMEM((1, SLOTS), jnp.int32),
            pltpu.SMEM((1, SLOTS), jnp.int32),
            pltpu.SMEM((NC, NR), jnp.int32),
            pltpu.VMEM((1, SLOTS), jnp.int32),
            pltpu.VMEM((1, SLOTS), jnp.int32),
            *[pltpu.VMEM((M, *tile), F32)] * 7,
            pltpu.VMEM((2, M // 2, *pair), I16),
            pltpu.VMEM((2, 1, LANES), F32),
            pltpu.VMEM((2, NC, M // 2, *pair), I16),
            pltpu.VMEM((2, NC, 1, LANES), F32),
            pltpu.VMEM((2, NR, M // 2, *pair), I16),
            pltpu.VMEM((2, NR, 1, LANES), F32),
            pltpu.VMEM((NC + NR, *tile), F32),
            pltpu.VMEM((RB, *pair), BF16),
            pltpu.VMEM((CB, *pair), BF16),
            pltpu.VMEM((RB, 2 * SLOTS), BF16),
            pltpu.VMEM((CB, 2 * SLOTS), BF16),
            pltpu.VMEM((2, *tile), F32),
            pltpu.VMEM((K * SLOTS, LANES), F32),
            pltpu.VMEM((K * SLOTS, LANES), F32),
            pltpu.VMEM((2, NC, K // 2, *pair), I16),
            pltpu.VMEM((2, NR, K // 2, *pair), I16),
            pltpu.VMEM((2, 1, LANES), F32),
            pltpu.VMEM((2, 1, LANES), F32),
            pltpu.VMEM((2, NC, K // 2, *pair), I16),
            pltpu.VMEM((2, NR, K // 2, *pair), I16),
            pltpu.VMEM((2, NC, 1, LANES), F32),
            pltpu.VMEM((2, NR, 1, LANES), F32),
            pltpu.VMEM((K * M, LANES), F32),
            pltpu.VMEM((2, 1, LANES), F32),
            pltpu.VMEM((2, NR * NC, 1, LANES), F32),
            pltpu.VMEM((2, 1, LANES), F32),
            pltpu.VMEM((NR, 1, LANES), F32),
            pltpu.VMEM((NC, 1, LANES), F32),
            pltpu.SemaphoreType.DMA((10,)),
            pltpu.SemaphoreType.DMA((20,)),
            pltpu.SemaphoreType.DMA((20,)),
        ],
        compiler_params=pltpu.CompilerParams(
            collective_id=0, has_side_effects=True, vmem_limit_bytes=48 * 1024 * 1024
        ),
        name="lanczos",
    )(*[pltpu.with_memory_space_constraint(v, pltpu.HBM) for v in args])


def solution(mesh):
    assert mesh.shape["row"] == NR and mesh.shape["col"] == NC
    both = ("row", "col")
    return jax.shard_map(
        per_device,
        mesh=mesh,
        in_specs=(
            P(None, both),
            P("row", "col", None, None, None),
            P(None, "col", None),
            P(None, "col", None),
            P(),
        ),
        out_specs=(P(None, both), P()),
        check_vma=False,
    )
```

```python
import math

import jax
import jax.numpy as jnp
from jax import lax
from jax.experimental import pallas as pl
from jax.experimental.pallas import tpu as pltpu
from jax.sharding import PartitionSpec as P

F32 = jnp.float32
BF16 = jnp.bfloat16
MESH = pl.DeviceIdType.MESH

K = 8
LANES = 128
M = 8
SIDE = 4
NR, NC = 16, 8
RB, CB = NC * M, NR * M
SLOTS = 128
BATCH = 4
UNROLL = 32
I16 = jnp.int16
TOP = 32700.0
TINY = 1e-30


def bcast(x):
    return jnp.broadcast_to(x, (K, LANES))


def kernel(
    x_hbm, blocks, rows_hbm, cols_hbm, counts_hbm,
    next_out, tri_out,
    bl, blt, x_in, rows_s, cols_s, counts_s, rows_v, cols_v, xb, yb, yraw, zb, wb, q1, q2,
    own_q, own_s, seg_qr, seg_sr, seg_qc, seg_sc, spread, vr, vc, picks_r, picks_c, most, res_d, res_t,
    tot_r, tot_c, sum_sr, sum_sc, in_r, in_c, in_sr, in_sc, ykb, msg, ar, first, first_r, first_c,
    load_sem, send_sem, recv_sem,
):
    r = lax.axis_index("row")
    c = lax.axis_index("col")
    row_iota = lax.broadcasted_iota(jnp.int32, (K, LANES), 0)
    lane_iota = lax.broadcasted_iota(jnp.int32, (K, LANES), 1)

    def far(off):
        return -sum(min(d, SIDE - d) for d in off[:3]), off

    z0, x0 = r // SIDE, lax.rem(r, SIDE)
    y0, p0 = c // 2, lax.rem(c, 2)
    row_at = {
        (dz, dx): lax.rem(z0 + dz, SIDE) * SIDE + lax.rem(x0 + dx, SIDE) if dz + dx else r
        for dz in range(SIDE)
        for dx in range(SIDE)
    }
    col_at = {
        (dy, dp): lax.rem(y0 + dy, SIDE) * 2 + lax.rem(p0 + dp, 2) if dy + dp else c
        for dy in range(SIDE)
        for dp in range(2)
    }
    offsets = sorted(
        ((dz, dx, dy, dp) for dz, dx in row_at for dy, dp in col_at if dz + dx + dy + dp), key=far
    )
    others = [(row_at[o[:2]], col_at[o[2:]]) for o in offsets]
    row_peers = [row_at[o[:2]] for o in offsets if o[2:] == (0, 0)]
    col_peers = [col_at[o[2:]] for o in offsets if o[:2] == (0, 0)]

    barrier = pltpu.get_barrier_semaphore()
    for rr in row_peers:
        pl.semaphore_signal(barrier, inc=1, device_id=(rr, c), device_id_type=MESH)
    for cc in col_peers:
        pl.semaphore_signal(barrier, inc=1, device_id=(r, cc), device_id_type=MESH)

    parts = 4
    step = SLOTS // parts
    loads = [
        pltpu.make_async_copy(
            blocks.at[0, 0, pl.ds(i * step, step)], bl.at[pl.ds(i * step, step)], load_sem.at[i]
        )
        for i in range(parts)
    ]
    small = [
        pltpu.make_async_copy(src, dst, load_sem.at[parts + i])
        for i, (src, dst) in enumerate(
            [
                (x_hbm, x_in),
                (rows_hbm.at[r], rows_s),
                (cols_hbm.at[r], cols_s),
                (counts_hbm, counts_s),
                (rows_hbm.at[r], rows_v),
                (cols_hbm.at[r], cols_v),
            ]
        )
    ]
    for load in small + loads:
        load.start()

    def send(src, dst, sems, dev):
        pltpu.make_async_remote_copy(
            src_ref=src, dst_ref=dst, send_sem=send_sem.at[sems], recv_sem=recv_sem.at[sems],
            device_id=dev, device_id_type=MESH,
        ).start()

    def wait_bytes(ref, sem):
        pltpu.make_async_copy(ref, ref, sem).wait()

    def gram(a_ref, b_ref, lane0, tile):
        for j in range(K):
            acc = None
            for b in range(M):
                term = a_ref[b] * b_ref[b, pl.ds(j, 1), :]
                acc = term if acc is None else acc + term
            col = jnp.sum(acc, axis=1, keepdims=True)
            tile = jnp.where(lane_iota == 2 * K * row_iota + (lane0 + j), bcast(col), tile)
        return tile

    def tree(terms):
        while len(terms) > 1:
            terms = [p + q for p, q in zip(terms[::2], terms[1::2])]
        return terms[0]

    def first_reduce_start(tile):
        first[0] = jnp.sum(tile, axis=0, keepdims=True)
        for rr in row_peers:
            send(first.at[0], first_r.at[r], 18, (rr, c))

    def first_reduce_turn():
        wait_bytes(first_r.at[pl.ds(0, NR - 1)], recv_sem.at[18])
        first_r[r] = first[0]
        first[1] = tree([first_r[i] for i in range(NR)])
        for cc in col_peers:
            send(first.at[1], first_c.at[c], 19, (r, cc))

    def first_reduce_finish():
        wait_bytes(first_c.at[pl.ds(0, NC - 1)], recv_sem.at[19])
        first_c[c] = first[1]
        return bcast(tree([first_c[i] for i in range(NC)]))

    def reduce_start(n, tile):
        msg[n] = jnp.sum(tile, axis=0, keepdims=True)
        for dev in others:
            send(msg.at[n], ar.at[n, r * NC + c], 16 + n, dev)

    def reduce_finish(n):
        wait_bytes(ar.at[n, pl.ds(0, NR * NC - 1)], recv_sem.at[16 + n])
        ar[n, r * NC + c] = msg[n]
        sums = [ar[n, i] for i in range(8)]
        for i in range(8, NR * NC):
            sums[i % 8] = sums[i % 8] + ar[n, i]
        return bcast(tree(sums))

    def picked(total, lanes):
        return bcast(jnp.sum(jnp.where(lane_iota == lanes, total, 0.0), axis=1, keepdims=True))

    def columns(total, lane0):
        return [picked(total, 2 * K * row_iota + (lane0 + j)) for j in range(K)]

    def rows_of(total):
        return [picked(total, row_iota + 2 * K * j) for j in range(K)]

    def factor(gcols):
        g = list(gcols)
        d = [jnp.where(row_iota == m, 1.0, 0.0).astype(F32) for m in range(K)]
        unit = []
        diag = g[0]
        for j in range(K):
            inv = 1.0 / g[j][j : j + 1, :]
            f = jnp.where(row_iota > j, g[j] * inv, 0.0)
            unit.append(f + jnp.where(row_iota == j, 1.0, 0.0))
            if j:
                diag = jnp.where(row_iota == j, g[j], diag)
            for m in range(j + 1, K):
                g[m] = g[m] - f * g[m][j : j + 1, :]
            for m in range(j + 1):
                d[m] = d[m] - f * d[m][j : j + 1, :]
        root = jnp.sqrt(diag)
        rs = 1.0 / root
        inverse = [v * rs for v in d]
        upper = [jnp.where(row_iota <= m, g[m], 0.0) * rs for m in range(K)]
        lower = [unit[j] * root[j : j + 1, :] for j in range(K)]
        return inverse, upper, lower

    def matmul_cols(left, right):
        out = []
        for m in range(K):
            acc = left[0] * right[m][0:1, :]
            for p in range(1, K):
                acc = acc + left[p] * right[m][p : p + 1, :]
            out.append(acc)
        return out

    def apply(cols, ref, i):
        acc = cols[0] * ref[i, pl.ds(0, 1), :]
        for j in range(1, K):
            acc = acc + cols[j] * ref[i, pl.ds(j, 1), :]
        return acc

    zero = jnp.zeros((K, LANES), F32)
    zero_pair = jnp.zeros((2 * K, LANES), BF16)

    def cat(a, b, axis):
        return jnp.concatenate([a, b], axis=axis)

    def fixed(value):
        return jnp.round(value).astype(jnp.int32).astype(I16)

    def scales(largest):
        m = jnp.maximum(bcast(jnp.max(largest, axis=1, keepdims=True)), TINY)
        return TOP / m, m * (1.0 / TOP)

    def to_row(scale):
        return jnp.sum(jnp.where(lane_iota == row_iota, scale, 0.0), axis=0, keepdims=True)

    def unpack_scales(ref, count, at):
        for i in range(count):
            spread[at + i] = picked(bcast(ref[i]), row_iota)

    def quantise(src, n):
        largest = jnp.abs(src[0])
        for b in range(1, M):
            largest = jnp.maximum(largest, jnp.abs(src[b]))
        inv, scale = scales(largest)
        for bb in range(M // 2):
            own_q[n, bb] = fixed(cat(src[2 * bb] * inv, src[2 * bb + 1] * inv, 0))
        own_s[n] = to_row(scale)

    def gather_start(n):
        for cc in col_peers:
            send(own_s.at[n], seg_sr.at[n, c], 8 * n + 0, (r, cc))
        for cc in col_peers:
            send(own_q.at[n], seg_qr.at[n, c], 8 * n + 1, (r, cc))
        for rr in row_peers:
            send(own_s.at[n], seg_sc.at[n, r], 8 * n + 2, (rr, c))
        for rr in row_peers:
            send(own_q.at[n], seg_qc.at[n, r], 8 * n + 3, (rr, c))
        seg_sr[n, c] = own_s[n]
        seg_qr[n, c] = own_q[n]
        seg_sc[n, r] = own_s[n]
        seg_qc[n, r] = own_q[n]

    def split(pieces, quant, at, vec, group):
        def body(i, carry):
            for u in range(group):
                p = group * i + u
                scale = spread[at + p]
                for bb in range(M // 2):
                    both = quant[p, bb].astype(jnp.int32).astype(F32)
                    for h in range(2):
                        value = both[K * h : K * h + K] * scale
                        high = value.astype(BF16).astype(F32)
                        vec[M * p + 2 * bb + h] = cat(value, value - high, 0).astype(BF16)
            return carry

        lax.fori_loop(0, pieces // group, body, 0)

    def gather_row_segment(n):
        wait_bytes(seg_sr.at[n, pl.ds(0, NC - 1)], recv_sem.at[8 * n + 0])
        unpack_scales(seg_sr.at[n], NC, 0)
        wait_bytes(seg_qr.at[n, pl.ds(0, NC - 1)], recv_sem.at[8 * n + 1])
        split(NC, seg_qr.at[n], 0, vr, 4)

    def gather_col_segment(n):
        wait_bytes(seg_sc.at[n, pl.ds(0, NR - 1)], recv_sem.at[8 * n + 2])
        unpack_scales(seg_sc.at[n], NR, NC)
        wait_bytes(seg_qc.at[n, pl.ds(0, NR - 1)], recv_sem.at[8 * n + 3])
        split(NR, seg_qc.at[n], NC, vc, 4)

    def product(vec, ids, mats, res):
        count = counts_s[c, r]

        def body(q, largest):
            base = BATCH * q
            b = [mats[base + i] for i in range(BATCH)]
            tile = cat(cat(b[0], b[1], 0), cat(b[2], b[3], 0), 1)
            x = [vec[ids[0, base + i]] for i in range(BATCH)]
            lhs = jnp.concatenate(
                [
                    cat(zero_pair, x[i], 1) if i % 2 else cat(x[i], zero_pair, 1)
                    for i in range(BATCH)
                ],
                axis=0,
            )
            out = jnp.dot(lhs, tile, preferred_element_type=F32)
            for i in range(BATCH):
                half = LANES * (i // 2)
                part = out[2 * K * i : 2 * K * i + 2 * K, half : half + LANES]
                part = part[:K] + part[K:]
                res[pl.ds(base + i, K, stride=SLOTS), :] = part
                largest = jnp.maximum(largest, jnp.where(base + i < count, jnp.abs(part), 0.0))
            return largest

        return lax.fori_loop(0, SLOTS // BATCH, body, zero, unroll=UNROLL)

    def scatter(pick, res, inv, tot, pieces):
        for kk in range(K // 2):
            full = cat(
                res[pl.ds(2 * kk * SLOTS, SLOTS), :], res[pl.ds((2 * kk + 1) * SLOTS, SLOTS), :], 1
            )
            hi = full.astype(BF16)
            lo = (full - hi.astype(F32)).astype(BF16)
            out = jnp.dot(pick[...], cat(hi, lo, 0), preferred_element_type=F32)
            even = bcast(inv[2 * kk : 2 * kk + 1, :])
            odd = bcast(inv[2 * kk + 1 : 2 * kk + 2, :])
            for i in range(pieces):
                rows = out[M * i : M * i + M]
                tot[i, kk] = fixed(cat(rows[:, :LANES] * even, rows[:, LANES:] * odd, 0))

    def exchange_cols(n, largest):
        inv, scale = scales(largest * most[1])
        sum_sc[n] = to_row(scale)
        for rr in row_peers:
            send(sum_sc.at[n], in_sc.at[n, r], 8 * n + 4, (rr, c))
        scatter(picks_c, res_t, inv, tot_c.at[n], NR)
        for rr in row_peers:
            send(tot_c.at[n, rr], in_c.at[n, r], 8 * n + 5, (rr, c))
        in_sc[n, r] = sum_sc[n]
        in_c[n, r] = tot_c[n, r]

    def exchange_rows(n, largest):
        inv, scale = scales(largest * most[0])
        sum_sr[n] = to_row(scale)
        for cc in col_peers:
            send(sum_sr.at[n], in_sr.at[n, c], 8 * n + 6, (r, cc))
        scatter(picks_r, res_d, inv, tot_r.at[n], NC)
        for cc in col_peers:
            send(tot_r.at[n, cc], in_r.at[n, c], 8 * n + 7, (r, cc))
        in_sr[n, c] = sum_sr[n]
        in_r[n, c] = tot_r[n, c]

    def exchange_finish(n, out_ref):
        wait_bytes(in_sr.at[n, pl.ds(0, NC - 1)], recv_sem.at[8 * n + 6])
        wait_bytes(in_sc.at[n, pl.ds(0, NR - 1)], recv_sem.at[8 * n + 4])
        unpack_scales(in_sr.at[n], NC, 0)
        unpack_scales(in_sc.at[n], NR, NC)

        def term(ref, i, kk, at):
            even = bcast(spread[at + i, pl.ds(2 * kk, 1), :])
            odd = bcast(spread[at + i, pl.ds(2 * kk + 1, 1), :])
            return ref[n, i, kk].astype(jnp.int32).astype(F32) * cat(even, odd, 0)

        wait_bytes(in_r.at[n, pl.ds(0, NC - 1)], recv_sem.at[8 * n + 7])
        for kk in range(K // 2):
            terms = [term(in_r, i, kk, 0) for i in range(NC)]
            ykb[pl.ds(2 * M * kk, 2 * M), :] = tree(terms)
        wait_bytes(in_c.at[n, pl.ds(0, NR - 1)], recv_sem.at[8 * n + 5])
        for kk in range(K // 2):
            terms = [term(in_c, i, kk, NC) for i in range(NR)]
            ykb[pl.ds(2 * M * kk, 2 * M), :] += tree(terms)
        for b in range(M):
            out_ref[b] = ykb[pl.ds(b, K, stride=M), :]

    for load in small:
        load.wait()
    for b in range(M):
        xb[b] = x_in[:, pl.ds(LANES * b, LANES)]
    start_tile = gram(xb, xb, 0, zero)
    quantise(xb, 0)

    giota = lax.broadcasted_iota(jnp.int32, (1, SLOTS), 1)
    row_ids = rows_v[...]
    col_ids = cols_v[...]
    valid = giota < counts_s[c, r]
    global_row = r * RB + row_ids
    global_col = ((col_ids // M) * NC + c) * M + lax.rem(col_ids, M)
    mirror = jnp.logical_and(valid, global_row != global_col)
    want_r = jnp.where(valid, row_ids, -1)
    want_c = jnp.where(mirror, col_ids, -1)
    one_r = jnp.where(lax.broadcasted_iota(jnp.int32, (RB, SLOTS), 0) == want_r, 1.0, 0.0)
    one_c = jnp.where(lax.broadcasted_iota(jnp.int32, (CB, SLOTS), 0) == want_c, 1.0, 0.0)
    for i, one in enumerate((one_r, one_c)):
        most[i] = bcast(jnp.max(jnp.sum(one, axis=1, keepdims=True), axis=0, keepdims=True))
    one_r = one_r.astype(BF16)
    one_c = one_c.astype(BF16)
    picks_r[...] = cat(one_r, one_r, 1)
    picks_c[...] = cat(one_c, one_c, 1)

    pl.semaphore_wait(barrier, NR + NC - 2)

    first_reduce_start(start_tile)
    gather_start(0)
    for load in loads:
        load.wait()

    def turn(i, carry):
        for u in range(8):
            blt[8 * i + u] = bl[8 * i + u].T
        return carry

    lax.fori_loop(0, SLOTS // 8, turn, 0)

    gather_row_segment(0)
    largest = product(vr, rows_s, bl, res_t)
    exchange_cols(0, largest)
    first_reduce_turn()
    gather_col_segment(0)
    largest = product(vc, cols_s, blt, res_d)
    exchange_rows(0, largest)
    inverse, _, _ = factor(columns(first_reduce_finish(), 0))
    for b in range(M):
        q1[b] = apply(inverse, xb, b)
    exchange_finish(0, yraw)
    for b in range(M):
        yb[b] = apply(inverse, yraw, b)

    quantise(yb, 1)
    gather_start(1)
    tile = gram(yb, q1, 0, zero)
    tile = gram(yb, yb, K, tile)
    reduce_start(0, tile)
    gather_row_segment(1)
    largest = product(vr, rows_s, bl, res_t)
    exchange_cols(1, largest)
    gather_col_segment(1)
    largest = product(vc, cols_s, blt, res_d)
    exchange_rows(1, largest)
    total = reduce_finish(0)
    at_cols = columns(total, 0)
    s_cols = columns(total, K)
    a1_cols = rows_of(total)
    ata = matmul_cols(at_cols, a1_cols)
    inverse, upper1, lower1 = factor([s - t for s, t in zip(s_cols, ata)])
    back = matmul_cols(inverse, at_cols)
    for b in range(M):
        q2[b] = apply(inverse, yb, b) - apply(back, q1, b)
        wb[b] = apply(back, yb, b) + apply(upper1, q1, b)
    top = zero
    for j in range(K):
        top = jnp.where(lane_iota == j, a1_cols[j], top)
        top = jnp.where(lane_iota == K + j, lower1[j], top)
    tri_out[pl.ds(0, K), :] = top[:, : 2 * K]
    exchange_finish(1, zb)
    for b in range(M):
        wb[b] = apply(inverse, zb, b) - wb[b]
    tile = gram(wb, q2, 0, zero)
    tile = gram(wb, wb, K, tile)
    reduce_start(1, tile)

    wait_bytes(first_r.at[pl.ds(0, NR - 1)], send_sem.at[18])
    wait_bytes(first_c.at[pl.ds(0, NC - 1)], send_sem.at[19])
    wait_bytes(ar.at[0, pl.ds(0, NR * NC - 1)], send_sem.at[16])
    for n in range(2):
        for i, (ref, count) in enumerate(
            [
                (seg_sr, NC), (seg_qr, NC), (seg_sc, NR), (seg_qc, NR),
                (in_sc, NR), (in_c, NR), (in_sr, NC), (in_r, NC),
            ]
        ):
            wait_bytes(ref.at[n, pl.ds(0, count - 1)], send_sem.at[8 * n + i])

    total = reduce_finish(1)
    at_cols = columns(total, 0)
    s_cols = columns(total, K)
    a2_cols = rows_of(total)
    ata = matmul_cols(at_cols, a2_cols)
    inverse, _, _ = factor([s - t for s, t in zip(s_cols, ata)])
    back = matmul_cols(inverse, at_cols)
    order_root = math.sqrt(NR * NC * M * LANES)
    for b in range(M):
        value = apply(inverse, wb, b) - apply(back, q2, b)
        next_out[:, pl.ds(LANES * b, LANES)] = value * order_root
    low = zero
    for j in range(K):
        low = jnp.where(lane_iota == j, upper1[j], low)
        low = jnp.where(lane_iota == K + j, a2_cols[j], low)
    tri_out[pl.ds(K, K), :] = low[:, : 2 * K]
    wait_bytes(ar.at[1, pl.ds(0, NR * NC - 1)], send_sem.at[17])


def write_out(block, projection, block_out, projection_out, sems):
    copies = [
        pltpu.make_async_copy(block, block_out, sems.at[0]),
        pltpu.make_async_copy(projection, projection_out, sems.at[1]),
    ]
    for copy in copies:
        copy.start()
    for copy in copies:
        copy.wait()


def per_device(start_block, blocks, block_rows, block_cols, counts):
    args = (start_block, blocks, block_rows, block_cols, counts.T)
    vmem = pl.BlockSpec(memory_space=pltpu.VMEM)
    hbm = pl.BlockSpec(memory_space=pltpu.HBM)
    tile = (K, LANES)
    pair = (2 * K, LANES)
    block, projection = pl.pallas_call(
        kernel,
        out_shape=(
            jax.ShapeDtypeStruct((K, M * LANES), F32),
            jax.ShapeDtypeStruct((2 * K, 2 * K), F32),
        ),
        in_specs=[hbm] * 5,
        out_specs=(vmem, vmem),
        scratch_shapes=[
            pltpu.VMEM((SLOTS, LANES, LANES), BF16),
            pltpu.VMEM((SLOTS, LANES, LANES), BF16),
            pltpu.VMEM((K, M * LANES), F32),
            pltpu.SMEM((1, SLOTS), jnp.int32),
            pltpu.SMEM((1, SLOTS), jnp.int32),
            pltpu.SMEM((NC, NR), jnp.int32),
            pltpu.VMEM((1, SLOTS), jnp.int32),
            pltpu.VMEM((1, SLOTS), jnp.int32),
            *[pltpu.VMEM((M, *tile), F32)] * 7,
            pltpu.VMEM((2, M // 2, *pair), I16),
            pltpu.VMEM((2, 1, LANES), F32),
            pltpu.VMEM((2, NC, M // 2, *pair), I16),
            pltpu.VMEM((2, NC, 1, LANES), F32),
            pltpu.VMEM((2, NR, M // 2, *pair), I16),
            pltpu.VMEM((2, NR, 1, LANES), F32),
            pltpu.VMEM((NC + NR, *tile), F32),
            pltpu.VMEM((RB, *pair), BF16),
            pltpu.VMEM((CB, *pair), BF16),
            pltpu.VMEM((RB, 2 * SLOTS), BF16),
            pltpu.VMEM((CB, 2 * SLOTS), BF16),
            pltpu.VMEM((2, *tile), F32),
            pltpu.VMEM((K * SLOTS, LANES), F32),
            pltpu.VMEM((K * SLOTS, LANES), F32),
            pltpu.VMEM((2, NC, K // 2, *pair), I16),
            pltpu.VMEM((2, NR, K // 2, *pair), I16),
            pltpu.VMEM((2, 1, LANES), F32),
            pltpu.VMEM((2, 1, LANES), F32),
            pltpu.VMEM((2, NC, K // 2, *pair), I16),
            pltpu.VMEM((2, NR, K // 2, *pair), I16),
            pltpu.VMEM((2, NC, 1, LANES), F32),
            pltpu.VMEM((2, NR, 1, LANES), F32),
            pltpu.VMEM((K * M, LANES), F32),
            pltpu.VMEM((2, 1, LANES), F32),
            pltpu.VMEM((2, NR * NC, 1, LANES), F32),
            pltpu.VMEM((2, 1, LANES), F32),
            pltpu.VMEM((NR, 1, LANES), F32),
            pltpu.VMEM((NC, 1, LANES), F32),
            pltpu.SemaphoreType.DMA((10,)),
            pltpu.SemaphoreType.DMA((20,)),
            pltpu.SemaphoreType.DMA((20,)),
        ],
        compiler_params=pltpu.CompilerParams(
            collective_id=0, has_side_effects=True, vmem_limit_bytes=48 * 1024 * 1024
        ),
        name="lanczos",
    )(*[pltpu.with_memory_space_constraint(v, pltpu.HBM) for v in args])
    return pl.pallas_call(
        write_out,
        out_shape=(
            jax.ShapeDtypeStruct(block.shape, F32),
            jax.ShapeDtypeStruct(projection.shape, F32),
        ),
        in_specs=[vmem, vmem],
        out_specs=(hbm, hbm),
        scratch_shapes=[pltpu.SemaphoreType.DMA((2,))],
        name="write_out",
    )(
        pltpu.with_memory_space_constraint(block, pltpu.VMEM),
        pltpu.with_memory_space_constraint(projection, pltpu.VMEM),
    )


def solution(mesh):
    assert mesh.shape["row"] == NR and mesh.shape["col"] == NC
    both = ("row", "col")
    return jax.shard_map(
        per_device,
        mesh=mesh,
        in_specs=(
            P(None, both),
            P("row", "col", None, None, None),
            P(None, "col", None),
            P(None, "col", None),
            P(),
        ),
        out_specs=(P(None, both), P()),
        check_vma=False,
    )
```

```python
import math

import jax
import jax.numpy as jnp
from jax import lax
from jax.experimental import pallas as pl
from jax.experimental.pallas import tpu as pltpu
from jax.sharding import PartitionSpec as P

F32 = jnp.float32
BF16 = jnp.bfloat16
MESH = pl.DeviceIdType.MESH

K = 8
LANES = 128
M = 8
SIDE = 4
NR, NC = 16, 8
RB, CB = NC * M, NR * M
SLOTS = 128
BATCH = 4
UNROLL = 32
PITCH = 132
I16 = jnp.int16
TOP = 32700.0
TINY = 1e-30


def bcast(x):
    return jnp.broadcast_to(x, (K, LANES))


def kernel(
    x_hbm, blocks, rows_hbm, cols_hbm, counts_hbm,
    next_out, tri_out,
    bl, blt, x_in, ids_s, counts_s, ids_v, xb, yb, yraw, zb, wb, q1, q2,
    own_q, own_s, seg_qr, seg_sr, seg_qc, seg_sc, spread, vr, vc, picks_r, picks_c, most, res_d, res_t,
    tot_r, tot_c, sum_sr, sum_sc, in_r, in_c, in_sr, in_sc, ykb, msg, ar, first, first_r, first_c,
    load_sem, send_sem, recv_sem,
):
    r = lax.axis_index("row")
    c = lax.axis_index("col")
    row_iota = lax.broadcasted_iota(jnp.int32, (K, LANES), 0)
    lane_iota = lax.broadcasted_iota(jnp.int32, (K, LANES), 1)

    def far(off):
        return -sum(min(d, SIDE - d) for d in off[:3]), off

    z0, x0 = r // SIDE, lax.rem(r, SIDE)
    y0, p0 = c // 2, lax.rem(c, 2)
    row_at = {
        (dz, dx): lax.rem(z0 + dz, SIDE) * SIDE + lax.rem(x0 + dx, SIDE) if dz + dx else r
        for dz in range(SIDE)
        for dx in range(SIDE)
    }
    col_at = {
        (dy, dp): lax.rem(y0 + dy, SIDE) * 2 + lax.rem(p0 + dp, 2) if dy + dp else c
        for dy in range(SIDE)
        for dp in range(2)
    }
    offsets = sorted(
        ((dz, dx, dy, dp) for dz, dx in row_at for dy, dp in col_at if dz + dx + dy + dp), key=far
    )
    others = [(row_at[o[:2]], col_at[o[2:]]) for o in offsets]
    row_peers = [row_at[o[:2]] for o in offsets if o[2:] == (0, 0)]
    col_peers = [col_at[o[2:]] for o in offsets if o[:2] == (0, 0)]

    barrier = pltpu.get_barrier_semaphore()
    for rr in row_peers:
        pl.semaphore_signal(barrier, inc=1, device_id=(rr, c), device_id_type=MESH)
    for cc in col_peers:
        pl.semaphore_signal(barrier, inc=1, device_id=(r, cc), device_id_type=MESH)

    parts = 4
    step = SLOTS // parts
    small = [
        pltpu.make_async_copy(src, dst, load_sem.at[i])
        for src, dst, i in [
            (x_hbm, x_in, 0),
            (rows_hbm.at[r], ids_v.at[0], 1),
            (cols_hbm.at[r], ids_v.at[1], 1),
            (rows_hbm.at[r], ids_s.at[0], 2),
            (cols_hbm.at[r], ids_s.at[1], 2),
            (counts_hbm, counts_s, 3),
        ]
    ]
    loads = [
        pltpu.make_async_copy(
            blocks.at[0, 0, pl.ds(i * step, step)], bl.at[pl.ds(i * step, step)], load_sem.at[4]
        )
        for i in range(parts)
    ]
    for load in small + loads:
        load.start()

    def send(src, dst, sems, dev):
        kind = 2 if sems >= 18 else 1 if sems >= 16 else 1 - sems % 2
        pltpu.make_async_remote_copy(
            src_ref=src, dst_ref=dst, send_sem=send_sem.at[kind], recv_sem=recv_sem.at[sems],
            device_id=dev, device_id_type=MESH,
        ).start()

    def wait_bytes(ref, sem):
        pltpu.make_async_copy(ref, ref, sem).wait()

    def send_if(wanted, *copy):
        @pl.when(wanted)
        def _():
            send(*copy)

    def wait_pieces(ref, sem, count):
        for i in range(1, NR):

            @pl.when(count == i)
            def _():
                wait_bytes(ref.at[pl.ds(0, i)], sem)

    def gram(a_ref, b_ref, lane0, tile):
        for j in range(K):
            acc = None
            for b in range(M):
                term = a_ref[b] * b_ref[b, pl.ds(j, 1), :]
                acc = term if acc is None else acc + term
            col = jnp.sum(acc, axis=1, keepdims=True)
            tile = jnp.where(lane_iota == 2 * K * row_iota + (lane0 + j), bcast(col), tile)
        return tile

    def tree(terms):
        while len(terms) > 1:
            terms = [p + q for p, q in zip(terms[::2], terms[1::2])]
        return terms[0]

    def first_reduce_start(tile):
        first[0] = jnp.sum(tile, axis=0, keepdims=True)
        for rr in row_peers:
            send(first.at[0], first_r.at[r], 18, (rr, c))

    def first_reduce_turn():
        wait_bytes(first_r.at[pl.ds(0, NR - 1)], recv_sem.at[18])
        first_r[r] = first[0]
        first[1] = tree([first_r[i] for i in range(NR)])
        for cc in col_peers:
            send(first.at[1], first_c.at[c], 19, (r, cc))

    def first_reduce_finish():
        wait_bytes(first_c.at[pl.ds(0, NC - 1)], recv_sem.at[19])
        first_c[c] = first[1]
        return bcast(tree([first_c[i] for i in range(NC)]))

    def reduce_start(n, tile):
        msg[n] = jnp.sum(tile, axis=0, keepdims=True)
        for dev in others:
            send(msg.at[n], ar.at[n, r * NC + c], 16 + n, dev)

    def reduce_finish(n):
        wait_bytes(ar.at[n, pl.ds(0, NR * NC - 1)], recv_sem.at[16 + n])
        ar[n, r * NC + c] = msg[n]
        sums = [ar[n, i] for i in range(8)]
        for i in range(8, NR * NC):
            sums[i % 8] = sums[i % 8] + ar[n, i]
        return bcast(tree(sums))

    def picked(total, lanes):
        return bcast(jnp.sum(jnp.where(lane_iota == lanes, total, 0.0), axis=1, keepdims=True))

    def columns(total, lane0):
        return [picked(total, 2 * K * row_iota + (lane0 + j)) for j in range(K)]

    def rows_of(total):
        return [picked(total, row_iota + 2 * K * j) for j in range(K)]

    def factor(gcols):
        g = list(gcols)
        d = [jnp.where(row_iota == m, 1.0, 0.0).astype(F32) for m in range(K)]
        unit = []
        diag = g[0]
        for j in range(K):
            inv = 1.0 / g[j][j : j + 1, :]
            f = jnp.where(row_iota > j, g[j] * inv, 0.0)
            unit.append(f + jnp.where(row_iota == j, 1.0, 0.0))
            if j:
                diag = jnp.where(row_iota == j, g[j], diag)
            for m in range(j + 1, K):
                g[m] = g[m] - f * g[m][j : j + 1, :]
            for m in range(j + 1):
                d[m] = d[m] - f * d[m][j : j + 1, :]
        root = jnp.sqrt(diag)
        rs = 1.0 / root
        inverse = [v * rs for v in d]
        upper = [jnp.where(row_iota <= m, g[m], 0.0) * rs for m in range(K)]
        lower = [unit[j] * root[j : j + 1, :] for j in range(K)]
        return inverse, upper, lower

    def matmul_cols(left, right):
        out = []
        for m in range(K):
            acc = left[0] * right[m][0:1, :]
            for p in range(1, K):
                acc = acc + left[p] * right[m][p : p + 1, :]
            out.append(acc)
        return out

    def apply(cols, ref, i):
        acc = cols[0] * ref[i, pl.ds(0, 1), :]
        for j in range(1, K):
            acc = acc + cols[j] * ref[i, pl.ds(j, 1), :]
        return acc

    zero = jnp.zeros((K, LANES), F32)
    zero_pair = jnp.zeros((2 * K, LANES), BF16)

    def cat(a, b, axis):
        return jnp.concatenate([a, b], axis=axis)

    def fixed(value):
        return jnp.round(value).astype(jnp.int32).astype(I16)

    def scales(largest):
        m = jnp.maximum(bcast(jnp.max(largest, axis=1, keepdims=True)), TINY)
        return TOP / m, m * (1.0 / TOP)

    def to_row(scale):
        return jnp.sum(jnp.where(lane_iota == row_iota, scale, 0.0), axis=0, keepdims=True)

    def unpack_scales(ref, count, at):
        for i in range(count):
            spread[at + i] = picked(bcast(ref[i]), row_iota)

    def quantise(src, n):
        largest = jnp.abs(src[0])
        for b in range(1, M):
            largest = jnp.maximum(largest, jnp.abs(src[b]))
        inv, scale = scales(largest)
        for bb in range(M // 2):
            own_q[n, bb] = fixed(cat(src[2 * bb] * inv, src[2 * bb + 1] * inv, 0))
        own_s[n] = to_row(scale)

    def gather_start(n):
        for cc in col_peers:
            send(own_s.at[n], seg_sr.at[n, c], 8 * n + 0, (r, cc))
        for cc in col_peers:
            send(own_q.at[n], seg_qr.at[n, c], 8 * n + 1, (r, cc))
        for rr in row_peers:
            send_if(rr > r, own_s.at[n], seg_sc.at[n, r], 8 * n + 2, (rr, c))
        for rr in row_peers:
            send_if(rr > r, own_q.at[n], seg_qc.at[n, r], 8 * n + 3, (rr, c))
        seg_sr[n, c] = own_s[n]
        seg_qr[n, c] = own_q[n]
        seg_sc[n, r] = own_s[n]
        seg_qc[n, r] = own_q[n]

    def split(pieces, quant, at, vec, group):
        def body(i, carry):
            for u in range(group):
                p = group * i + u
                scale = spread[at + p]
                for bb in range(M // 2):
                    both = quant[p, bb].astype(jnp.int32).astype(F32)
                    for h in range(2):
                        value = both[K * h : K * h + K] * scale
                        high = value.astype(BF16).astype(F32)
                        vec[M * p + 2 * bb + h] = cat(value, value - high, 0).astype(BF16)
            return carry

        lax.fori_loop(0, pieces // group, body, 0)

    def gather_row_segment(n):
        wait_bytes(seg_sr.at[n, pl.ds(0, NC - 1)], recv_sem.at[8 * n + 0])
        unpack_scales(seg_sr.at[n], NC, 0)
        wait_bytes(seg_qr.at[n, pl.ds(0, NC - 1)], recv_sem.at[8 * n + 1])
        split(NC, seg_qr.at[n], 0, vr, 4)

    def gather_col_scales(n):
        wait_pieces(seg_sc.at[n], recv_sem.at[8 * n + 2], r)
        unpack_scales(seg_sc.at[n], NR, NC)

    def gather_col_segment(n):
        wait_pieces(seg_qc.at[n], recv_sem.at[8 * n + 3], r)
        split(NR, seg_qc.at[n], NC, vc, 4)

    def product(vec, which, mats, res):
        count = counts_s[c, r]

        def body(q, largest):
            base = BATCH * q
            b = [mats[base + i] for i in range(BATCH)]
            tile = cat(cat(b[0], b[1], 0), cat(b[2], b[3], 0), 1)
            x = [vec[ids_s[which, 0, base + i]] for i in range(BATCH)]
            lhs = jnp.concatenate(
                [
                    cat(zero_pair, x[i], 1) if i % 2 else cat(x[i], zero_pair, 1)
                    for i in range(BATCH)
                ],
                axis=0,
            )
            out = jnp.dot(lhs, tile, preferred_element_type=F32)
            for i in range(BATCH):
                half = LANES * (i // 2)
                part = out[2 * K * i : 2 * K * i + 2 * K, half : half + LANES]
                part = part[:K] + part[K:]
                res[pl.ds(base + i, K, stride=PITCH), :] = part
                largest = jnp.maximum(largest, jnp.where(base + i < count, jnp.abs(part), 0.0))
            return largest

        return lax.fori_loop(0, SLOTS // BATCH, body, zero, unroll=UNROLL)

    def scatter(pick, res, inv, tot, pieces):
        for kk in range(K // 2):
            full = cat(
                res[pl.ds(2 * kk * PITCH, SLOTS), :], res[pl.ds((2 * kk + 1) * PITCH, SLOTS), :], 1
            )
            hi = full.astype(BF16)
            lo = (full - hi.astype(F32)).astype(BF16)
            out = jnp.dot(pick[...], cat(hi, lo, 0), preferred_element_type=F32)
            even = bcast(inv[2 * kk : 2 * kk + 1, :])
            odd = bcast(inv[2 * kk + 1 : 2 * kk + 2, :])
            for i in range(pieces):
                rows = out[M * i : M * i + M]
                tot[i, kk] = fixed(cat(rows[:, :LANES] * even, rows[:, LANES:] * odd, 0))

    def exchange_cols(n, largest):
        inv, scale = scales(largest * most[1])
        sum_sc[n] = to_row(scale)
        for rr in row_peers:
            send_if(rr < r, sum_sc.at[n], in_sc.at[n, r], 8 * n + 4, (rr, c))
        scatter(picks_c, res_t, inv, tot_c.at[n], NR)
        for rr in row_peers:
            send_if(rr < r, tot_c.at[n, rr], in_c.at[n, r], 8 * n + 5, (rr, c))
        in_sc[n, r] = sum_sc[n]
        in_c[n, r] = tot_c[n, r]

    def exchange_rows(n, largest):
        inv, scale = scales(largest * most[0])
        sum_sr[n] = to_row(scale)
        for cc in col_peers:
            send(sum_sr.at[n], in_sr.at[n, c], 8 * n + 6, (r, cc))
        scatter(picks_r, res_d, inv, tot_r.at[n], NC)
        for cc in col_peers:
            send(tot_r.at[n, cc], in_r.at[n, c], 8 * n + 7, (r, cc))
        in_sr[n, c] = sum_sr[n]
        in_r[n, c] = tot_r[n, c]

    def exchange_finish(n, out_ref):
        wait_bytes(in_sr.at[n, pl.ds(0, NC - 1)], recv_sem.at[8 * n + 6])
        wait_pieces(in_sc.at[n], recv_sem.at[8 * n + 4], NR - 1 - r)
        unpack_scales(in_sr.at[n], NC, 0)
        unpack_scales(in_sc.at[n], NR, NC)

        def term(ref, i, kk, at):
            even = bcast(spread[at + i, pl.ds(2 * kk, 1), :])
            odd = bcast(spread[at + i, pl.ds(2 * kk + 1, 1), :])
            return ref[n, i, kk].astype(jnp.int32).astype(F32) * cat(even, odd, 0)

        wait_bytes(in_r.at[n, pl.ds(0, NC - 1)], recv_sem.at[8 * n + 7])
        for kk in range(K // 2):
            terms = [term(in_r, i, kk, 0) for i in range(NC)]
            ykb[pl.ds(2 * M * kk, 2 * M), :] = tree(terms)
        wait_pieces(in_c.at[n], recv_sem.at[8 * n + 5], NR - 1 - r)
        for kk in range(K // 2):
            terms = [term(in_c, i, kk, NC) for i in range(NR)]
            ykb[pl.ds(2 * M * kk, 2 * M), :] += tree(terms)
        for b in range(M):
            out_ref[b] = ykb[pl.ds(b, K, stride=M), :]

    for i, ref in enumerate((x_in, ids_v, ids_s, counts_s)):
        wait_bytes(ref, load_sem.at[i])
    for b in range(M):
        xb[b] = x_in[:, pl.ds(LANES * b, LANES)]
    start_tile = gram(xb, xb, 0, zero)
    quantise(xb, 0)

    giota = lax.broadcasted_iota(jnp.int32, (1, SLOTS), 1)
    row_ids = ids_v[0]
    col_ids = ids_v[1]
    valid = giota < counts_s[c, r]
    global_row = r * RB + row_ids
    global_col = ((col_ids // M) * NC + c) * M + lax.rem(col_ids, M)
    mirror = jnp.logical_and(valid, global_row != global_col)
    want_r = jnp.where(valid, row_ids, -1)
    want_c = jnp.where(mirror, col_ids, -1)
    one_r = jnp.where(lax.broadcasted_iota(jnp.int32, (RB, SLOTS), 0) == want_r, 1.0, 0.0)
    one_c = jnp.where(lax.broadcasted_iota(jnp.int32, (CB, SLOTS), 0) == want_c, 1.0, 0.0)
    for i, one in enumerate((one_r, one_c)):
        most[i] = bcast(jnp.max(jnp.sum(one, axis=1, keepdims=True), axis=0, keepdims=True))
    one_r = one_r.astype(BF16)
    one_c = one_c.astype(BF16)
    picks_r[...] = cat(one_r, one_r, 1)
    picks_c[...] = cat(one_c, one_c, 1)

    pl.semaphore_wait(barrier, NR + NC - 2)

    first_reduce_start(start_tile)
    gather_start(0)
    wait_bytes(bl, load_sem.at[4])

    def turn(i, carry):
        for u in range(8):
            blt[8 * i + u] = bl[8 * i + u].T
        return carry

    lax.fori_loop(0, SLOTS // 8, turn, 0)

    def clear(refs, i, wanted):
        @pl.when(wanted)
        def _():
            for ref in refs:
                for n in range(2):
                    ref[n, i] = jnp.zeros_like(ref[n, i])

    for i in range(NR):
        clear((in_c, in_sc), i, r > i)
        clear((seg_qc, seg_sc), i, r < i)

    gather_row_segment(0)
    largest = product(vr, 0, bl, res_t)
    first_reduce_turn()
    exchange_cols(0, largest)
    gather_col_scales(0)
    gather_col_segment(0)
    largest = product(vc, 1, blt, res_d)
    exchange_rows(0, largest)
    inverse, _, _ = factor(columns(first_reduce_finish(), 0))
    for b in range(M):
        q1[b] = apply(inverse, xb, b)
    exchange_finish(0, yraw)
    for b in range(M):
        yb[b] = apply(inverse, yraw, b)

    quantise(yb, 1)
    gather_start(1)
    tile = gram(yb, q1, 0, zero)
    tile = gram(yb, yb, K, tile)
    reduce_start(0, tile)
    gather_row_segment(1)
    largest = product(vr, 0, bl, res_t)
    exchange_cols(1, largest)
    gather_col_scales(1)
    gather_col_segment(1)
    largest = product(vc, 1, blt, res_d)
    exchange_rows(1, largest)
    total = reduce_finish(0)
    at_cols = columns(total, 0)
    s_cols = columns(total, K)
    a1_cols = rows_of(total)
    ata = matmul_cols(at_cols, a1_cols)
    inverse, upper1, lower1 = factor([s - t for s, t in zip(s_cols, ata)])
    back = matmul_cols(inverse, at_cols)
    for b in range(M):
        q2[b] = apply(inverse, yb, b) - apply(back, q1, b)
        wb[b] = apply(back, yb, b) + apply(upper1, q1, b)
    top = zero
    for j in range(K):
        top = jnp.where(lane_iota == j, a1_cols[j], top)
        top = jnp.where(lane_iota == K + j, lower1[j], top)
    tri_out[pl.ds(0, K), :] = top[:, : 2 * K]
    exchange_finish(1, zb)
    for b in range(M):
        wb[b] = apply(inverse, zb, b) - wb[b]
    tile = gram(wb, q2, 0, zero)
    tile = gram(wb, wb, K, tile)
    reduce_start(1, tile)

    total = reduce_finish(1)
    at_cols = columns(total, 0)
    s_cols = columns(total, K)
    a2_cols = rows_of(total)
    ata = matmul_cols(at_cols, a2_cols)
    for b in range(M):
        wb[b] = wb[b] - apply(at_cols, q2, b)
    order_root = math.sqrt(NR * NC * M * LANES)
    inverse, _, _ = factor([s - t for s, t in zip(s_cols, ata)])
    inverse = [v * order_root for v in inverse]
    for b in range(M):
        next_out[:, pl.ds(LANES * b, LANES)] = apply(inverse, wb, b)
    low = zero
    for j in range(K):
        low = jnp.where(lane_iota == j, upper1[j], low)
        low = jnp.where(lane_iota == K + j, a2_cols[j], low)
    tri_out[pl.ds(K, K), :] = low[:, : 2 * K]

    sent = 2 * (2 * (NC - 1) + NR - 1)
    wait_bytes(bl.at[pl.ds(0, sent // 2)], send_sem.at[0])
    wait_bytes(res_d.at[pl.ds(0, sent + 2 * (NR * NC - 1))], send_sem.at[1])
    wait_bytes(ar.at[0, pl.ds(0, NR + NC - 2)], send_sem.at[2])


def write_out(block, projection, block_out, projection_out, sems):
    copies = [
        pltpu.make_async_copy(block, block_out, sems.at[0]),
        pltpu.make_async_copy(projection, projection_out, sems.at[1]),
    ]
    for copy in copies:
        copy.start()
    for copy in copies:
        copy.wait()


def per_device(start_block, blocks, block_rows, block_cols, counts):
    args = (start_block, blocks, block_rows, block_cols, counts.T)
    vmem = pl.BlockSpec(memory_space=pltpu.VMEM)
    hbm = pl.BlockSpec(memory_space=pltpu.HBM)
    tile = (K, LANES)
    pair = (2 * K, LANES)
    block, projection = pl.pallas_call(
        kernel,
        out_shape=(
            jax.ShapeDtypeStruct((K, M * LANES), F32),
            jax.ShapeDtypeStruct((2 * K, 2 * K), F32),
        ),
        in_specs=[hbm] * 5,
        out_specs=(vmem, vmem),
        scratch_shapes=[
            pltpu.VMEM((SLOTS, LANES, LANES), BF16),
            pltpu.VMEM((SLOTS, LANES, LANES), BF16),
            pltpu.VMEM((K, M * LANES), F32),
            pltpu.SMEM((2, 1, SLOTS), jnp.int32),
            pltpu.SMEM((NC, NR), jnp.int32),
            pltpu.VMEM((2, 1, SLOTS), jnp.int32),
            *[pltpu.VMEM((M, *tile), F32)] * 7,
            pltpu.VMEM((2, M // 2, *pair), I16),
            pltpu.VMEM((2, 1, LANES), F32),
            pltpu.VMEM((2, NC, M // 2, *pair), I16),
            pltpu.VMEM((2, NC, 1, LANES), F32),
            pltpu.VMEM((2, NR, M // 2, *pair), I16),
            pltpu.VMEM((2, NR, 1, LANES), F32),
            pltpu.VMEM((NC + NR, *tile), F32),
            pltpu.VMEM((RB, *pair), BF16),
            pltpu.VMEM((CB, *pair), BF16),
            pltpu.VMEM((RB, 2 * SLOTS), BF16),
            pltpu.VMEM((CB, 2 * SLOTS), BF16),
            pltpu.VMEM((2, *tile), F32),
            pltpu.VMEM((K * PITCH, LANES), F32),
            pltpu.VMEM((K * PITCH, LANES), F32),
            pltpu.VMEM((2, NC, K // 2, *pair), I16),
            pltpu.VMEM((2, NR, K // 2, *pair), I16),
            pltpu.VMEM((2, 1, LANES), F32),
            pltpu.VMEM((2, 1, LANES), F32),
            pltpu.VMEM((2, NC, K // 2, *pair), I16),
            pltpu.VMEM((2, NR, K // 2, *pair), I16),
            pltpu.VMEM((2, NC, 1, LANES), F32),
            pltpu.VMEM((2, NR, 1, LANES), F32),
            pltpu.VMEM((K * M, LANES), F32),
            pltpu.VMEM((2, 1, LANES), F32),
            pltpu.VMEM((2, NR * NC, 1, LANES), F32),
            pltpu.VMEM((2, 1, LANES), F32),
            pltpu.VMEM((NR, 1, LANES), F32),
            pltpu.VMEM((NC, 1, LANES), F32),
            pltpu.SemaphoreType.DMA((5,)),
            pltpu.SemaphoreType.DMA((20,)),
            pltpu.SemaphoreType.DMA((20,)),
        ],
        compiler_params=pltpu.CompilerParams(
            collective_id=0, has_side_effects=True, vmem_limit_bytes=48 * 1024 * 1024
        ),
        name="lanczos",
    )(*[pltpu.with_memory_space_constraint(v, pltpu.HBM) for v in args])
    return pl.pallas_call(
        write_out,
        out_shape=(
            jax.ShapeDtypeStruct(block.shape, F32),
            jax.ShapeDtypeStruct(projection.shape, F32),
        ),
        in_specs=[vmem, vmem],
        out_specs=(hbm, hbm),
        scratch_shapes=[pltpu.SemaphoreType.DMA((2,))],
        name="write_out",
    )(
        pltpu.with_memory_space_constraint(block, pltpu.VMEM),
        pltpu.with_memory_space_constraint(projection, pltpu.VMEM),
    )


def solution(mesh):
    assert mesh.shape["row"] == NR and mesh.shape["col"] == NC
    both = ("row", "col")
    return jax.shard_map(
        per_device,
        mesh=mesh,
        in_specs=(
            P(None, both),
            P("row", "col", None, None, None),
            P(None, "col", None),
            P(None, "col", None),
            P(),
        ),
        out_specs=(P(None, both), P()),
        check_vma=False,
    )
```

```python
import math

import jax
import jax.numpy as jnp
from jax import lax
from jax.experimental import pallas as pl
from jax.experimental.pallas import tpu as pltpu
from jax.sharding import PartitionSpec as P

F32 = jnp.float32
BF16 = jnp.bfloat16
MESH = pl.DeviceIdType.MESH

K = 8
LANES = 128
M = 8
SIDE = 4
NR, NC = 16, 8
RB, CB = NC * M, NR * M
SLOTS = 128
BATCH = 4
UNROLL = 32
PITCH = 132
I16 = jnp.int16
TOP = 32700.0
TINY = 1e-30


def bcast(x):
    return jnp.broadcast_to(x, (K, LANES))


def kernel(
    x_hbm, blocks, rows_hbm, cols_hbm, counts_hbm,
    next_out, tri_out,
    bl, blt, x_in, ids_s, counts_s, ids_v, xb, yb, yraw, zb, wb, q1, q2,
    own_q, own_s, seg_qr, seg_sr, seg_qc, seg_sc, spread, vr, vc, picks_r, picks_c, most, res_d, res_t,
    tot_r, tot_c, sum_sr, sum_sc, in_r, in_c, in_sr, in_sc, ykb, msg, ar, first, first_r, first_c,
    load_sem, send_sem, recv_sem,
):
    r = lax.axis_index("row")
    c = lax.axis_index("col")
    row_iota = lax.broadcasted_iota(jnp.int32, (K, LANES), 0)
    lane_iota = lax.broadcasted_iota(jnp.int32, (K, LANES), 1)

    def far(off):
        return -sum(min(d, SIDE - d) for d in off[:3]), off

    z0, x0 = r // SIDE, lax.rem(r, SIDE)
    y0, p0 = c // 2, lax.rem(c, 2)
    row_at = {
        (dz, dx): lax.rem(z0 + dz, SIDE) * SIDE + lax.rem(x0 + dx, SIDE) if dz + dx else r
        for dz in range(SIDE)
        for dx in range(SIDE)
    }
    col_at = {
        (dy, dp): lax.rem(y0 + dy, SIDE) * 2 + lax.rem(p0 + dp, 2) if dy + dp else c
        for dy in range(SIDE)
        for dp in range(2)
    }
    offsets = sorted(
        ((dz, dx, dy, dp) for dz, dx in row_at for dy, dp in col_at if dz + dx + dy + dp), key=far
    )
    others = [(row_at[o[:2]], col_at[o[2:]]) for o in offsets]
    row_peers = [row_at[o[:2]] for o in offsets if o[2:] == (0, 0)]
    col_peers = [col_at[o[2:]] for o in offsets if o[:2] == (0, 0)]

    barrier = pltpu.get_barrier_semaphore()
    for rr in row_peers:
        pl.semaphore_signal(barrier, inc=1, device_id=(rr, c), device_id_type=MESH)
    for cc in col_peers:
        pl.semaphore_signal(barrier, inc=1, device_id=(r, cc), device_id_type=MESH)

    parts = 4
    step = SLOTS // parts
    small = [
        pltpu.make_async_copy(src, dst, load_sem.at[i])
        for src, dst, i in [
            (x_hbm, x_in, 0),
            (rows_hbm.at[r], ids_v.at[0], 1),
            (cols_hbm.at[r], ids_v.at[1], 1),
            (rows_hbm.at[r], ids_s.at[0], 2),
            (cols_hbm.at[r], ids_s.at[1], 2),
            (counts_hbm, counts_s, 3),
        ]
    ]
    loads = [
        pltpu.make_async_copy(
            blocks.at[0, 0, pl.ds(i * step, step)], bl.at[pl.ds(i * step, step)], load_sem.at[4]
        )
        for i in range(parts)
    ]
    for load in small + loads:
        load.start()

    def send(src, dst, sems, dev):
        kind = 2 if sems >= 18 else 1 if sems >= 16 else 1 - sems % 2
        pltpu.make_async_remote_copy(
            src_ref=src, dst_ref=dst, send_sem=send_sem.at[kind], recv_sem=recv_sem.at[sems],
            device_id=dev, device_id_type=MESH,
        ).start()

    def wait_bytes(ref, sem):
        pltpu.make_async_copy(ref, ref, sem).wait()

    def send_if(wanted, *copy):
        @pl.when(wanted)
        def _():
            send(*copy)

    def wait_pieces(ref, sem, count):
        for i in range(1, NR):

            @pl.when(count == i)
            def _():
                wait_bytes(ref.at[pl.ds(0, i)], sem)

    def gram(a_ref, b_ref, lane0, tile):
        for j in range(K):
            acc = None
            for b in range(M):
                term = a_ref[b] * b_ref[b, pl.ds(j, 1), :]
                acc = term if acc is None else acc + term
            col = jnp.sum(acc, axis=1, keepdims=True)
            tile = jnp.where(lane_iota == 2 * K * row_iota + (lane0 + j), bcast(col), tile)
        return tile

    def tree(terms):
        while len(terms) > 1:
            terms = [p + q for p, q in zip(terms[::2], terms[1::2])]
        return terms[0]

    def first_reduce_start(tile):
        first[0] = jnp.sum(tile, axis=0, keepdims=True)
        for rr in row_peers:
            send(first.at[0], first_r.at[r], 18, (rr, c))

    def first_reduce_turn():
        wait_bytes(first_r.at[pl.ds(0, NR - 1)], recv_sem.at[18])
        first_r[r] = first[0]
        first[1] = tree([first_r[i] for i in range(NR)])
        for cc in col_peers:
            send(first.at[1], first_c.at[c], 19, (r, cc))

    def first_reduce_finish():
        wait_bytes(first_c.at[pl.ds(0, NC - 1)], recv_sem.at[19])
        first_c[c] = first[1]
        return bcast(tree([first_c[i] for i in range(NC)]))

    def reduce_start(n, tile):
        msg[n] = jnp.sum(tile, axis=0, keepdims=True)
        for dev in others:
            send(msg.at[n], ar.at[n, r * NC + c], 16 + n, dev)

    def reduce_finish(n):
        wait_bytes(ar.at[n, pl.ds(0, NR * NC - 1)], recv_sem.at[16 + n])
        ar[n, r * NC + c] = msg[n]
        sums = [ar[n, i] for i in range(8)]
        for i in range(8, NR * NC):
            sums[i % 8] = sums[i % 8] + ar[n, i]
        return bcast(tree(sums))

    def picked(total, lanes):
        return bcast(jnp.sum(jnp.where(lane_iota == lanes, total, 0.0), axis=1, keepdims=True))

    def columns(total, lane0):
        return [picked(total, 2 * K * row_iota + (lane0 + j)) for j in range(K)]

    def rows_of(total):
        return [picked(total, row_iota + 2 * K * j) for j in range(K)]

    def factor(gcols):
        g = list(gcols)
        d = [jnp.where(row_iota == m, 1.0, 0.0).astype(F32) for m in range(K)]
        unit = []
        diag = g[0]
        for j in range(K):
            inv = 1.0 / g[j][j : j + 1, :]
            f = jnp.where(row_iota > j, g[j] * inv, 0.0)
            unit.append(f + jnp.where(row_iota == j, 1.0, 0.0))
            if j:
                diag = jnp.where(row_iota == j, g[j], diag)
            for m in range(j + 1, K):
                g[m] = g[m] - f * g[m][j : j + 1, :]
            for m in range(j + 1):
                d[m] = d[m] - f * d[m][j : j + 1, :]
        root = jnp.sqrt(diag)
        rs = 1.0 / root
        inverse = [v * rs for v in d]
        upper = [jnp.where(row_iota <= m, g[m], 0.0) * rs for m in range(K)]
        lower = [unit[j] * root[j : j + 1, :] for j in range(K)]
        return inverse, upper, lower

    def matmul_cols(left, right):
        out = []
        for m in range(K):
            acc = left[0] * right[m][0:1, :]
            for p in range(1, K):
                acc = acc + left[p] * right[m][p : p + 1, :]
            out.append(acc)
        return out

    def apply(cols, ref, i):
        acc = cols[0] * ref[i, pl.ds(0, 1), :]
        for j in range(1, K):
            acc = acc + cols[j] * ref[i, pl.ds(j, 1), :]
        return acc

    zero = jnp.zeros((K, LANES), F32)
    zero_pair = jnp.zeros((2 * K, LANES), BF16)

    def cat(a, b, axis):
        return jnp.concatenate([a, b], axis=axis)

    def fixed(value):
        return jnp.round(value).astype(jnp.int32).astype(I16)

    def scales(largest):
        m = jnp.maximum(bcast(jnp.max(largest, axis=1, keepdims=True)), TINY)
        return TOP / m, m * (1.0 / TOP)

    def to_row(scale):
        return jnp.sum(jnp.where(lane_iota == row_iota, scale, 0.0), axis=0, keepdims=True)

    def unpack_scales(ref, count, at):
        for i in range(count):
            spread[at + i] = picked(bcast(ref[i]), row_iota)

    def quantise(src, n):
        largest = jnp.abs(src[0])
        for b in range(1, M):
            largest = jnp.maximum(largest, jnp.abs(src[b]))
        inv, scale = scales(largest)
        for bb in range(M // 2):
            own_q[n, bb] = fixed(cat(src[2 * bb] * inv, src[2 * bb + 1] * inv, 0))
        own_s[n] = to_row(scale)

    def gather_start(n):
        for cc in col_peers:
            send(own_s.at[n], seg_sr.at[n, c], 8 * n + 0, (r, cc))
        for cc in col_peers:
            send(own_q.at[n], seg_qr.at[n, c], 8 * n + 1, (r, cc))
        for rr in row_peers:

            @pl.when(rr > r)
            def _():
                send(own_s.at[n], seg_sc.at[n, r], 8 * n + 2, (rr, c))
                send(own_q.at[n], seg_qc.at[n, r], 8 * n + 3, (rr, c))

        seg_sr[n, c] = own_s[n]
        seg_qr[n, c] = own_q[n]
        seg_sc[n, r] = own_s[n]
        seg_qc[n, r] = own_q[n]

    def split(pieces, quant, at, vec, group):
        def body(i, carry):
            for u in range(group):
                p = group * i + u
                scale = spread[at + p]
                for bb in range(M // 2):
                    both = quant[p, bb].astype(jnp.int32).astype(F32)
                    for h in range(2):
                        value = both[K * h : K * h + K] * scale
                        high = value.astype(BF16).astype(F32)
                        vec[M * p + 2 * bb + h] = cat(value, value - high, 0).astype(BF16)
            return carry

        lax.fori_loop(0, pieces // group, body, 0)

    def gather_row_segment(n):
        wait_bytes(seg_sr.at[n, pl.ds(0, NC - 1)], recv_sem.at[8 * n + 0])
        unpack_scales(seg_sr.at[n], NC, 0)
        wait_bytes(seg_qr.at[n, pl.ds(0, NC - 1)], recv_sem.at[8 * n + 1])
        split(NC, seg_qr.at[n], 0, vr, 4)

    def gather_col_scales(n):
        wait_pieces(seg_sc.at[n], recv_sem.at[8 * n + 2], r)
        unpack_scales(seg_sc.at[n], NR, NC)

    def gather_col_segment(n):
        wait_pieces(seg_qc.at[n], recv_sem.at[8 * n + 3], r)
        split(NR, seg_qc.at[n], NC, vc, 4)

    def product(vec, which, mats, res):
        count = counts_s[c, r]

        def body(q, largest):
            base = BATCH * q
            b = [mats[base + i] for i in range(BATCH)]
            tile = cat(cat(b[0], b[1], 0), cat(b[2], b[3], 0), 1)
            x = [vec[ids_s[which, 0, base + i]] for i in range(BATCH)]
            lhs = jnp.concatenate(
                [
                    cat(zero_pair, x[i], 1) if i % 2 else cat(x[i], zero_pair, 1)
                    for i in range(BATCH)
                ],
                axis=0,
            )
            out = jnp.dot(lhs, tile, preferred_element_type=F32)
            for i in range(BATCH):
                half = LANES * (i // 2)
                part = out[2 * K * i : 2 * K * i + 2 * K, half : half + LANES]
                part = part[:K] + part[K:]
                res[pl.ds(base + i, K, stride=PITCH), :] = part
                largest = jnp.maximum(largest, jnp.where(base + i < count, jnp.abs(part), 0.0))
            return largest

        return lax.fori_loop(0, SLOTS // BATCH, body, zero, unroll=UNROLL)

    def scatter(pick, res, inv, tot, pieces):
        for kk in range(K // 2):
            full = cat(
                res[pl.ds(2 * kk * PITCH, SLOTS), :], res[pl.ds((2 * kk + 1) * PITCH, SLOTS), :], 1
            )
            hi = full.astype(BF16)
            lo = (full - hi.astype(F32)).astype(BF16)
            out = jnp.dot(pick[...], cat(hi, lo, 0), preferred_element_type=F32)
            even = bcast(inv[2 * kk : 2 * kk + 1, :])
            odd = bcast(inv[2 * kk + 1 : 2 * kk + 2, :])
            for i in range(pieces):
                rows = out[M * i : M * i + M]
                tot[i, kk] = fixed(cat(rows[:, :LANES] * even, rows[:, LANES:] * odd, 0))

    def exchange_cols(n, largest):
        inv, scale = scales(largest * most[1])
        sum_sc[n] = to_row(scale)
        scatter(picks_c, res_t, inv, tot_c.at[n], NR)
        for rr in row_peers:

            @pl.when(rr < r)
            def _():
                send(sum_sc.at[n], in_sc.at[n, r], 8 * n + 4, (rr, c))
                send(tot_c.at[n, rr], in_c.at[n, r], 8 * n + 5, (rr, c))

        in_sc[n, r] = sum_sc[n]
        in_c[n, r] = tot_c[n, r]

    def exchange_rows(n, largest):
        inv, scale = scales(largest * most[0])
        sum_sr[n] = to_row(scale)
        for cc in col_peers:
            send(sum_sr.at[n], in_sr.at[n, c], 8 * n + 6, (r, cc))
        scatter(picks_r, res_d, inv, tot_r.at[n], NC)
        for cc in col_peers:
            send(tot_r.at[n, cc], in_r.at[n, c], 8 * n + 7, (r, cc))
        in_sr[n, c] = sum_sr[n]
        in_r[n, c] = tot_r[n, c]

    def exchange_finish(n, out_ref):
        wait_bytes(in_sr.at[n, pl.ds(0, NC - 1)], recv_sem.at[8 * n + 6])
        wait_pieces(in_sc.at[n], recv_sem.at[8 * n + 4], NR - 1 - r)
        unpack_scales(in_sr.at[n], NC, 0)
        unpack_scales(in_sc.at[n], NR, NC)

        def term(ref, i, kk, at):
            even = bcast(spread[at + i, pl.ds(2 * kk, 1), :])
            odd = bcast(spread[at + i, pl.ds(2 * kk + 1, 1), :])
            return ref[n, i, kk].astype(jnp.int32).astype(F32) * cat(even, odd, 0)

        wait_bytes(in_r.at[n, pl.ds(0, NC - 1)], recv_sem.at[8 * n + 7])
        for kk in range(K // 2):
            terms = [term(in_r, i, kk, 0) for i in range(NC)]
            ykb[pl.ds(2 * M * kk, 2 * M), :] = tree(terms)
        wait_pieces(in_c.at[n], recv_sem.at[8 * n + 5], NR - 1 - r)
        for kk in range(K // 2):
            terms = [term(in_c, i, kk, NC) for i in range(NR)]
            ykb[pl.ds(2 * M * kk, 2 * M), :] += tree(terms)
        for b in range(M):
            out_ref[b] = ykb[pl.ds(b, K, stride=M), :]

    for i, ref in enumerate((x_in, ids_v, ids_s, counts_s)):
        wait_bytes(ref, load_sem.at[i])
    for b in range(M):
        xb[b] = x_in[:, pl.ds(LANES * b, LANES)]
    start_tile = gram(xb, xb, 0, zero)
    quantise(xb, 0)

    giota = lax.broadcasted_iota(jnp.int32, (1, SLOTS), 1)
    row_ids = ids_v[0]
    col_ids = ids_v[1]
    valid = giota < counts_s[c, r]
    global_row = r * RB + row_ids
    global_col = ((col_ids // M) * NC + c) * M + lax.rem(col_ids, M)
    mirror = jnp.logical_and(valid, global_row != global_col)
    want_r = jnp.where(valid, row_ids, -1)
    want_c = jnp.where(mirror, col_ids, -1)
    one_r = jnp.where(lax.broadcasted_iota(jnp.int32, (RB, SLOTS), 0) == want_r, 1.0, 0.0)
    one_c = jnp.where(lax.broadcasted_iota(jnp.int32, (CB, SLOTS), 0) == want_c, 1.0, 0.0)
    for i, one in enumerate((one_r, one_c)):
        most[i] = bcast(jnp.max(jnp.sum(one, axis=1, keepdims=True), axis=0, keepdims=True))
    one_r = one_r.astype(BF16)
    one_c = one_c.astype(BF16)
    picks_r[...] = cat(one_r, one_r, 1)
    picks_c[...] = cat(one_c, one_c, 1)

    pl.semaphore_wait(barrier, NR + NC - 2)

    first_reduce_start(start_tile)
    gather_start(0)
    wait_bytes(bl, load_sem.at[4])

    def turn(i, carry):
        for u in range(8):
            blt[8 * i + u] = bl[8 * i + u].T
        return carry

    lax.fori_loop(0, SLOTS // 8, turn, 0)

    def clear(refs, i, wanted):
        @pl.when(wanted)
        def _():
            for ref in refs:
                for n in range(2):
                    ref[n, i] = jnp.zeros_like(ref[n, i])

    for i in range(NR):
        clear((in_c, in_sc), i, r > i)
        clear((seg_qc, seg_sc), i, r < i)

    gather_row_segment(0)
    largest = product(vr, 0, bl, res_t)
    first_reduce_turn()
    exchange_cols(0, largest)
    gather_col_scales(0)
    gather_col_segment(0)
    largest = product(vc, 1, blt, res_d)
    exchange_rows(0, largest)
    inverse, _, _ = factor(columns(first_reduce_finish(), 0))
    for b in range(M):
        q1[b] = apply(inverse, xb, b)
    exchange_finish(0, yraw)
    for b in range(M):
        yb[b] = apply(inverse, yraw, b)

    quantise(yb, 1)
    gather_start(1)
    tile = gram(yb, q1, 0, zero)
    tile = gram(yb, yb, K, tile)
    reduce_start(0, tile)
    gather_row_segment(1)
    largest = product(vr, 0, bl, res_t)
    exchange_cols(1, largest)
    gather_col_scales(1)
    gather_col_segment(1)
    largest = product(vc, 1, blt, res_d)
    exchange_rows(1, largest)
    total = reduce_finish(0)
    at_cols = columns(total, 0)
    s_cols = columns(total, K)
    a1_cols = rows_of(total)
    ata = matmul_cols(at_cols, a1_cols)
    inverse, upper1, lower1 = factor([s - t for s, t in zip(s_cols, ata)])
    back = matmul_cols(inverse, at_cols)
    for b in range(M):
        q2[b] = apply(inverse, yb, b) - apply(back, q1, b)
        wb[b] = apply(back, yb, b) + apply(upper1, q1, b)
    top = zero
    for j in range(K):
        top = jnp.where(lane_iota == j, a1_cols[j], top)
        top = jnp.where(lane_iota == K + j, lower1[j], top)
    tri_out[pl.ds(0, K), :] = top[:, : 2 * K]
    exchange_finish(1, zb)
    for b in range(M):
        wb[b] = apply(inverse, zb, b) - wb[b]
    tile = gram(wb, q2, 0, zero)
    tile = gram(wb, wb, K, tile)
    reduce_start(1, tile)

    total = reduce_finish(1)
    at_cols = columns(total, 0)
    s_cols = columns(total, K)
    a2_cols = rows_of(total)
    ata = matmul_cols(at_cols, a2_cols)
    for b in range(M):
        wb[b] = wb[b] - apply(at_cols, q2, b)
    order_root = math.sqrt(NR * NC * M * LANES)
    inverse, _, _ = factor([s - t for s, t in zip(s_cols, ata)])
    inverse = [v * order_root for v in inverse]
    for b in range(M):
        next_out[:, pl.ds(LANES * b, LANES)] = apply(inverse, wb, b)
    low = zero
    for j in range(K):
        low = jnp.where(lane_iota == j, upper1[j], low)
        low = jnp.where(lane_iota == K + j, a2_cols[j], low)
    tri_out[pl.ds(K, K), :] = low[:, : 2 * K]

    sent = 2 * (2 * (NC - 1) + NR - 1)
    wait_bytes(bl.at[pl.ds(0, sent // 2)], send_sem.at[0])
    wait_bytes(res_d.at[pl.ds(0, sent + 2 * (NR * NC - 1))], send_sem.at[1])
    wait_bytes(ar.at[0, pl.ds(0, NR + NC - 2)], send_sem.at[2])


def write_out(block, projection, block_out, projection_out, sems):
    copies = [
        pltpu.make_async_copy(block, block_out, sems.at[0]),
        pltpu.make_async_copy(projection, projection_out, sems.at[1]),
    ]
    for copy in copies:
        copy.start()
    for copy in copies:
        copy.wait()


def per_device(start_block, blocks, block_rows, block_cols, counts):
    args = (start_block, blocks, block_rows, block_cols, counts.T)
    vmem = pl.BlockSpec(memory_space=pltpu.VMEM)
    hbm = pl.BlockSpec(memory_space=pltpu.HBM)
    tile = (K, LANES)
    pair = (2 * K, LANES)
    block, projection = pl.pallas_call(
        kernel,
        out_shape=(
            jax.ShapeDtypeStruct((K, M * LANES), F32),
            jax.ShapeDtypeStruct((2 * K, 2 * K), F32),
        ),
        in_specs=[hbm] * 5,
        out_specs=(vmem, vmem),
        scratch_shapes=[
            pltpu.VMEM((SLOTS, LANES, LANES), BF16),
            pltpu.VMEM((SLOTS, LANES, LANES), BF16),
            pltpu.VMEM((K, M * LANES), F32),
            pltpu.SMEM((2, 1, SLOTS), jnp.int32),
            pltpu.SMEM((NC, NR), jnp.int32),
            pltpu.VMEM((2, 1, SLOTS), jnp.int32),
            *[pltpu.VMEM((M, *tile), F32)] * 7,
            pltpu.VMEM((2, M // 2, *pair), I16),
            pltpu.VMEM((2, 1, LANES), F32),
            pltpu.VMEM((2, NC, M // 2, *pair), I16),
            pltpu.VMEM((2, NC, 1, LANES), F32),
            pltpu.VMEM((2, NR, M // 2, *pair), I16),
            pltpu.VMEM((2, NR, 1, LANES), F32),
            pltpu.VMEM((NC + NR, *tile), F32),
            pltpu.VMEM((RB, *pair), BF16),
            pltpu.VMEM((CB, *pair), BF16),
            pltpu.VMEM((RB, 2 * SLOTS), BF16),
            pltpu.VMEM((CB, 2 * SLOTS), BF16),
            pltpu.VMEM((2, *tile), F32),
            pltpu.VMEM(((K + 1) * PITCH, LANES), F32),
            pltpu.VMEM(((K + 1) * PITCH, LANES), F32),
            pltpu.VMEM((2, NC, K // 2, *pair), I16),
            pltpu.VMEM((2, NR, K // 2, *pair), I16),
            pltpu.VMEM((2, 1, LANES), F32),
            pltpu.VMEM((2, 1, LANES), F32),
            pltpu.VMEM((2, NC, K // 2, *pair), I16),
            pltpu.VMEM((2, NR, K // 2, *pair), I16),
            pltpu.VMEM((2, NC, 1, LANES), F32),
            pltpu.VMEM((2, NR, 1, LANES), F32),
            pltpu.VMEM(((K + 1) * M, LANES), F32),
            pltpu.VMEM((2, 1, LANES), F32),
            pltpu.VMEM((2, NR * NC, 1, LANES), F32),
            pltpu.VMEM((2, 1, LANES), F32),
            pltpu.VMEM((NR, 1, LANES), F32),
            pltpu.VMEM((NC, 1, LANES), F32),
            pltpu.SemaphoreType.DMA((5,)),
            pltpu.SemaphoreType.DMA((20,)),
            pltpu.SemaphoreType.DMA((20,)),
        ],
        compiler_params=pltpu.CompilerParams(
            collective_id=0, has_side_effects=True, vmem_limit_bytes=48 * 1024 * 1024
        ),
        name="lanczos",
    )(*[pltpu.with_memory_space_constraint(v, pltpu.HBM) for v in args])
    return pl.pallas_call(
        write_out,
        out_shape=(
            jax.ShapeDtypeStruct(block.shape, F32),
            jax.ShapeDtypeStruct(projection.shape, F32),
        ),
        in_specs=[vmem, vmem],
        out_specs=(hbm, hbm),
        scratch_shapes=[pltpu.SemaphoreType.DMA((2,))],
        name="write_out",
    )(
        pltpu.with_memory_space_constraint(block, pltpu.VMEM),
        pltpu.with_memory_space_constraint(projection, pltpu.VMEM),
    )


def solution(mesh):
    assert mesh.shape["row"] == NR and mesh.shape["col"] == NC
    both = ("row", "col")
    return jax.shard_map(
        per_device,
        mesh=mesh,
        in_specs=(
            P(None, both),
            P("row", "col", None, None, None),
            P(None, "col", None),
            P(None, "col", None),
            P(),
        ),
        out_specs=(P(None, both), P()),
        check_vma=False,
    )
```

```python
import math

import jax
import jax.numpy as jnp
from jax import lax
from jax.experimental import pallas as pl
from jax.experimental.pallas import tpu as pltpu
from jax.sharding import PartitionSpec as P

F32 = jnp.float32
BF16 = jnp.bfloat16
MESH = pl.DeviceIdType.MESH

K = 8
LANES = 128
M = 8
SIDE = 4
NR, NC = 16, 8
RB, CB = NC * M, NR * M
SLOTS = 128
BATCH = 4
UNROLL = 32
PITCH = 132
I16 = jnp.int16
TOP = 32700.0
TINY = 1e-30


def bcast(x):
    return jnp.broadcast_to(x, (K, LANES))


def kernel(
    x_hbm, blocks, rows_hbm, cols_hbm, counts_hbm,
    next_out, tri_out,
    bl, blt, x_in, ids_s, counts_s, ids_v, xb, yb, yraw, zb, wb, q1, q2,
    own_q, own_s, seg_qr, seg_sr, seg_qc, seg_sc, spread, vr, vc, picks_r, picks_c, most, res_d, res_t,
    tot_r, tot_c, sum_sr, sum_sc, in_r, in_c, in_sr, in_sc, ykb, msg, ar, first, first_r, first_c,
    load_sem, send_sem, recv_sem,
):
    r = lax.axis_index("row")
    c = lax.axis_index("col")
    row_iota = lax.broadcasted_iota(jnp.int32, (K, LANES), 0)
    lane_iota = lax.broadcasted_iota(jnp.int32, (K, LANES), 1)

    def far(off):
        return -sum(min(d, SIDE - d) for d in off[:3]), off

    z0, x0 = r // SIDE, lax.rem(r, SIDE)
    y0, p0 = c // 2, lax.rem(c, 2)
    row_at = {
        (dz, dx): lax.rem(z0 + dz, SIDE) * SIDE + lax.rem(x0 + dx, SIDE) if dz + dx else r
        for dz in range(SIDE)
        for dx in range(SIDE)
    }
    col_at = {
        (dy, dp): lax.rem(y0 + dy, SIDE) * 2 + lax.rem(p0 + dp, 2) if dy + dp else c
        for dy in range(SIDE)
        for dp in range(2)
    }
    offsets = sorted(
        ((dz, dx, dy, dp) for dz, dx in row_at for dy, dp in col_at if dz + dx + dy + dp), key=far
    )
    others = [(row_at[o[:2]], col_at[o[2:]]) for o in offsets]
    row_peers = [row_at[o[:2]] for o in offsets if o[2:] == (0, 0)]
    col_peers = [col_at[o[2:]] for o in offsets if o[:2] == (0, 0)]

    barrier = pltpu.get_barrier_semaphore()
    for rr in row_peers:
        pl.semaphore_signal(barrier, inc=1, device_id=(rr, c), device_id_type=MESH)
    for cc in col_peers:
        pl.semaphore_signal(barrier, inc=1, device_id=(r, cc), device_id_type=MESH)

    parts = 4
    step = SLOTS // parts
    small = [
        pltpu.make_async_copy(src, dst, load_sem.at[i])
        for src, dst, i in [
            (x_hbm, x_in, 0),
            (rows_hbm.at[r], ids_v.at[0], 1),
            (cols_hbm.at[r], ids_v.at[1], 1),
            (rows_hbm.at[r], ids_s.at[0], 2),
            (cols_hbm.at[r], ids_s.at[1], 2),
            (counts_hbm, counts_s, 3),
        ]
    ]
    loads = [
        pltpu.make_async_copy(
            blocks.at[0, 0, pl.ds(i * step, step)], bl.at[pl.ds(i * step, step)], load_sem.at[4]
        )
        for i in range(parts)
    ]
    for load in small + loads:
        load.start()

    def send(src, dst, sems, dev):
        kind = 2 if sems >= 18 else 1 if sems >= 16 else 1 - sems % 2
        pltpu.make_async_remote_copy(
            src_ref=src, dst_ref=dst, send_sem=send_sem.at[kind], recv_sem=recv_sem.at[sems],
            device_id=dev, device_id_type=MESH,
        ).start()

    def wait_bytes(ref, sem):
        pltpu.make_async_copy(ref, ref, sem).wait()

    def send_if(wanted, *copy):
        @pl.when(wanted)
        def _():
            send(*copy)

    def wait_pieces(ref, sem, count):
        for i in range(1, NR):

            @pl.when(count == i)
            def _():
                wait_bytes(ref.at[pl.ds(0, i)], sem)

    def gram(a_ref, b_ref, lane0, tile):
        for j in range(K):
            acc = None
            for b in range(M):
                term = a_ref[b] * b_ref[b, pl.ds(j, 1), :]
                acc = term if acc is None else acc + term
            col = jnp.sum(acc, axis=1, keepdims=True)
            tile = jnp.where(lane_iota == 2 * K * row_iota + (lane0 + j), bcast(col), tile)
        return tile

    def tree(terms):
        while len(terms) > 1:
            terms = [p + q for p, q in zip(terms[::2], terms[1::2])]
        return terms[0]

    def first_reduce_start(tile):
        first[0] = jnp.sum(tile, axis=0, keepdims=True)
        for rr in row_peers:
            send(first.at[0], first_r.at[r], 18, (rr, c))

    def first_reduce_turn():
        wait_bytes(first_r.at[pl.ds(0, NR - 1)], recv_sem.at[18])
        first_r[r] = first[0]
        first[1] = tree([first_r[i] for i in range(NR)])
        for cc in col_peers:
            send(first.at[1], first_c.at[c], 19, (r, cc))

    def first_reduce_finish():
        wait_bytes(first_c.at[pl.ds(0, NC - 1)], recv_sem.at[19])
        first_c[c] = first[1]
        return bcast(tree([first_c[i] for i in range(NC)]))

    def reduce_start(n, tile):
        msg[n] = jnp.sum(tile, axis=0, keepdims=True)
        for dev in others:
            send(msg.at[n], ar.at[n, r * NC + c], 16 + n, dev)

    def reduce_finish(n):
        wait_bytes(ar.at[n, pl.ds(0, NR * NC - 1)], recv_sem.at[16 + n])
        ar[n, r * NC + c] = msg[n]
        sums = [ar[n, i] for i in range(8)]
        for i in range(8, NR * NC):
            sums[i % 8] = sums[i % 8] + ar[n, i]
        return bcast(tree(sums))

    def picked(total, lanes):
        return bcast(jnp.sum(jnp.where(lane_iota == lanes, total, 0.0), axis=1, keepdims=True))

    def columns(total, lane0):
        return [picked(total, 2 * K * row_iota + (lane0 + j)) for j in range(K)]

    def rows_of(total):
        return [picked(total, row_iota + 2 * K * j) for j in range(K)]

    def factor(gcols):
        g = list(gcols)
        d = [jnp.where(row_iota == m, 1.0, 0.0).astype(F32) for m in range(K)]
        unit = []
        diag = g[0]
        for j in range(K):
            inv = 1.0 / g[j][j : j + 1, :]
            f = jnp.where(row_iota > j, g[j] * inv, 0.0)
            unit.append(f + jnp.where(row_iota == j, 1.0, 0.0))
            if j:
                diag = jnp.where(row_iota == j, g[j], diag)
            for m in range(j + 1, K):
                g[m] = g[m] - f * g[m][j : j + 1, :]
            for m in range(j + 1):
                d[m] = d[m] - f * d[m][j : j + 1, :]
        root = jnp.sqrt(diag)
        rs = 1.0 / root
        inverse = [v * rs for v in d]
        upper = [jnp.where(row_iota <= m, g[m], 0.0) * rs for m in range(K)]
        lower = [unit[j] * root[j : j + 1, :] for j in range(K)]
        return inverse, upper, lower

    def matmul_cols(left, right):
        out = []
        for m in range(K):
            acc = left[0] * right[m][0:1, :]
            for p in range(1, K):
                acc = acc + left[p] * right[m][p : p + 1, :]
            out.append(acc)
        return out

    def apply(cols, ref, i):
        acc = cols[0] * ref[i, pl.ds(0, 1), :]
        for j in range(1, K):
            acc = acc + cols[j] * ref[i, pl.ds(j, 1), :]
        return acc

    zero = jnp.zeros((K, LANES), F32)
    zero_pair = jnp.zeros((2 * K, LANES), BF16)

    def cat(a, b, axis):
        return jnp.concatenate([a, b], axis=axis)

    def fixed(value):
        return jnp.round(value).astype(jnp.int32).astype(I16)

    def scales(largest):
        m = jnp.maximum(bcast(jnp.max(largest, axis=1, keepdims=True)), TINY)
        return TOP / m, m * (1.0 / TOP)

    def to_row(scale):
        return jnp.sum(jnp.where(lane_iota == row_iota, scale, 0.0), axis=0, keepdims=True)

    def unpack_scales(ref, count, at):
        for i in range(count):
            spread[at + i] = picked(bcast(ref[i]), row_iota)

    def quantise(src, n):
        largest = jnp.abs(src[0])
        for b in range(1, M):
            largest = jnp.maximum(largest, jnp.abs(src[b]))
        inv, scale = scales(largest)
        for bb in range(M // 2):
            own_q[n, bb] = fixed(cat(src[2 * bb] * inv, src[2 * bb + 1] * inv, 0))
        own_s[n] = to_row(scale)

    def gather_start(n):
        for cc in col_peers:
            send(own_s.at[n], seg_sr.at[n, c], 8 * n + 0, (r, cc))
        for cc in col_peers:
            send(own_q.at[n], seg_qr.at[n, c], 8 * n + 1, (r, cc))
        for rr in row_peers:

            @pl.when(rr > r)
            def _():
                send(own_s.at[n], seg_sc.at[n, r], 8 * n + 2, (rr, c))
                send(own_q.at[n], seg_qc.at[n, r], 8 * n + 3, (rr, c))

        seg_sr[n, c] = own_s[n]
        seg_qr[n, c] = own_q[n]
        seg_sc[n, r] = own_s[n]
        seg_qc[n, r] = own_q[n]

    def split(pieces, quant, at, vec, group):
        def body(i, carry):
            for u in range(group):
                p = group * i + u
                scale = spread[at + p]
                for bb in range(M // 2):
                    both = quant[p, bb].astype(jnp.int32).astype(F32)
                    for h in range(2):
                        value = both[K * h : K * h + K] * scale
                        high = value.astype(BF16).astype(F32)
                        vec[M * p + 2 * bb + h] = cat(value, value - high, 0).astype(BF16)
            return carry

        lax.fori_loop(0, pieces // group, body, 0)

    def gather_row_segment(n):
        wait_bytes(seg_sr.at[n, pl.ds(0, NC - 1)], recv_sem.at[8 * n + 0])
        unpack_scales(seg_sr.at[n], NC, 0)
        wait_bytes(seg_qr.at[n, pl.ds(0, NC - 1)], recv_sem.at[8 * n + 1])
        split(NC, seg_qr.at[n], 0, vr, 8)

    def gather_col_scales(n):
        wait_pieces(seg_sc.at[n], recv_sem.at[8 * n + 2], r)
        unpack_scales(seg_sc.at[n], NR, NC)

    def gather_col_segment(n):
        wait_pieces(seg_qc.at[n], recv_sem.at[8 * n + 3], r)
        split(NR, seg_qc.at[n], NC, vc, 8)

    def product(vec, which, mats, res):
        count = counts_s[c, r]

        def body(q, largest):
            base = BATCH * q
            b = [mats[base + i] for i in range(BATCH)]
            tile = cat(cat(b[0], b[1], 0), cat(b[2], b[3], 0), 1)
            x = [vec[ids_s[which, 0, base + i]] for i in range(BATCH)]
            lhs = jnp.concatenate(
                [
                    cat(zero_pair, x[i], 1) if i % 2 else cat(x[i], zero_pair, 1)
                    for i in range(BATCH)
                ],
                axis=0,
            )
            out = jnp.dot(lhs, tile, preferred_element_type=F32)
            for i in range(BATCH):
                half = LANES * (i // 2)
                part = out[2 * K * i : 2 * K * i + 2 * K, half : half + LANES]
                part = part[:K] + part[K:]
                res[pl.ds(base + i, K, stride=PITCH), :] = part
                largest = jnp.maximum(largest, jnp.where(base + i < count, jnp.abs(part), 0.0))
            return largest

        return lax.fori_loop(0, SLOTS // BATCH, body, zero, unroll=UNROLL)

    def scatter(pick, res, inv, tot, pieces):
        for kk in range(K // 2):
            full = cat(
                res[pl.ds(2 * kk * PITCH, SLOTS), :], res[pl.ds((2 * kk + 1) * PITCH, SLOTS), :], 1
            )
            hi = full.astype(BF16)
            lo = (full - hi.astype(F32)).astype(BF16)
            out = jnp.dot(pick[...], cat(hi, lo, 0), preferred_element_type=F32)
            even = bcast(inv[2 * kk : 2 * kk + 1, :])
            odd = bcast(inv[2 * kk + 1 : 2 * kk + 2, :])
            for i in range(pieces):
                rows = out[M * i : M * i + M]
                tot[i, kk] = fixed(cat(rows[:, :LANES] * even, rows[:, LANES:] * odd, 0))

    def exchange_cols(n, largest):
        inv, scale = scales(largest * most[1])
        sum_sc[n] = to_row(scale)
        scatter(picks_c, res_t, inv, tot_c.at[n], NR)
        for rr in row_peers:

            @pl.when(rr < r)
            def _():
                send(sum_sc.at[n], in_sc.at[n, r], 8 * n + 4, (rr, c))
                send(tot_c.at[n, rr], in_c.at[n, r], 8 * n + 5, (rr, c))

        in_sc[n, r] = sum_sc[n]
        in_c[n, r] = tot_c[n, r]

    def exchange_rows(n, largest):
        inv, scale = scales(largest * most[0])
        sum_sr[n] = to_row(scale)
        for cc in col_peers:
            send(sum_sr.at[n], in_sr.at[n, c], 8 * n + 6, (r, cc))
        scatter(picks_r, res_d, inv, tot_r.at[n], NC)
        for cc in col_peers:
            send(tot_r.at[n, cc], in_r.at[n, c], 8 * n + 7, (r, cc))
        in_sr[n, c] = sum_sr[n]
        in_r[n, c] = tot_r[n, c]

    def exchange_finish(n, out_ref):
        wait_bytes(in_sr.at[n, pl.ds(0, NC - 1)], recv_sem.at[8 * n + 6])
        wait_pieces(in_sc.at[n], recv_sem.at[8 * n + 4], NR - 1 - r)
        unpack_scales(in_sr.at[n], NC, 0)
        unpack_scales(in_sc.at[n], NR, NC)

        def term(ref, i, kk, at):
            even = bcast(spread[at + i, pl.ds(2 * kk, 1), :])
            odd = bcast(spread[at + i, pl.ds(2 * kk + 1, 1), :])
            return ref[n, i, kk].astype(jnp.int32).astype(F32) * cat(even, odd, 0)

        wait_bytes(in_r.at[n, pl.ds(0, NC - 1)], recv_sem.at[8 * n + 7])
        for kk in range(K // 2):
            terms = [term(in_r, i, kk, 0) for i in range(NC)]
            ykb[pl.ds(2 * M * kk, 2 * M), :] = tree(terms)
        wait_pieces(in_c.at[n], recv_sem.at[8 * n + 5], NR - 1 - r)
        for kk in range(K // 2):
            terms = [term(in_c, i, kk, NC) for i in range(NR)]
            ykb[pl.ds(2 * M * kk, 2 * M), :] += tree(terms)
        for b in range(M):
            out_ref[b] = ykb[pl.ds(b, K, stride=M), :]

    for i, ref in enumerate((x_in, ids_v, ids_s, counts_s)):
        wait_bytes(ref, load_sem.at[i])
    for b in range(M):
        xb[b] = x_in[:, pl.ds(LANES * b, LANES)]
    start_tile = gram(xb, xb, 0, zero)
    quantise(xb, 0)

    giota = lax.broadcasted_iota(jnp.int32, (1, SLOTS), 1)
    row_ids = ids_v[0]
    col_ids = ids_v[1]
    valid = giota < counts_s[c, r]
    global_row = r * RB + row_ids
    global_col = ((col_ids // M) * NC + c) * M + lax.rem(col_ids, M)
    mirror = jnp.logical_and(valid, global_row != global_col)
    want_r = jnp.where(valid, row_ids, -1)
    want_c = jnp.where(mirror, col_ids, -1)
    one_r = jnp.where(lax.broadcasted_iota(jnp.int32, (RB, SLOTS), 0) == want_r, 1.0, 0.0)
    one_c = jnp.where(lax.broadcasted_iota(jnp.int32, (CB, SLOTS), 0) == want_c, 1.0, 0.0)
    for i, one in enumerate((one_r, one_c)):
        most[i] = bcast(jnp.max(jnp.sum(one, axis=1, keepdims=True), axis=0, keepdims=True))
    one_r = one_r.astype(BF16)
    one_c = one_c.astype(BF16)
    picks_r[...] = cat(one_r, one_r, 1)
    picks_c[...] = cat(one_c, one_c, 1)

    pl.semaphore_wait(barrier, NR + NC - 2)

    first_reduce_start(start_tile)
    gather_start(0)
    wait_bytes(bl, load_sem.at[4])

    def turn(i, carry):
        for u in range(8):
            blt[8 * i + u] = bl[8 * i + u].T
        return carry

    lax.fori_loop(0, SLOTS // 8, turn, 0)

    def clear(refs, i, wanted):
        @pl.when(wanted)
        def _():
            for ref in refs:
                for n in range(2):
                    ref[n, i] = jnp.zeros_like(ref[n, i])

    for i in range(NR):
        clear((in_c, in_sc), i, r > i)
        clear((seg_qc, seg_sc), i, r < i)

    gather_row_segment(0)
    largest = product(vr, 0, bl, res_t)
    first_reduce_turn()
    exchange_cols(0, largest)
    gather_col_scales(0)
    gather_col_segment(0)
    largest = product(vc, 1, blt, res_d)
    exchange_rows(0, largest)
    inverse, _, _ = factor(columns(first_reduce_finish(), 0))
    for b in range(M):
        q1[b] = apply(inverse, xb, b)
    exchange_finish(0, yraw)
    for b in range(M):
        yb[b] = apply(inverse, yraw, b)

    quantise(yb, 1)
    gather_start(1)
    tile = gram(yb, q1, 0, zero)
    tile = gram(yb, yb, K, tile)
    reduce_start(0, tile)
    gather_row_segment(1)
    largest = product(vr, 0, bl, res_t)
    exchange_cols(1, largest)
    gather_col_scales(1)
    gather_col_segment(1)
    largest = product(vc, 1, blt, res_d)
    exchange_rows(1, largest)
    total = reduce_finish(0)
    at_cols = columns(total, 0)
    s_cols = columns(total, K)
    a1_cols = rows_of(total)
    ata = matmul_cols(at_cols, a1_cols)
    inverse, upper1, lower1 = factor([s - t for s, t in zip(s_cols, ata)])
    back = matmul_cols(inverse, at_cols)
    for b in range(M):
        q2[b] = apply(inverse, yb, b) - apply(back, q1, b)
        wb[b] = apply(back, yb, b) + apply(upper1, q1, b)
    top = zero
    for j in range(K):
        top = jnp.where(lane_iota == j, a1_cols[j], top)
        top = jnp.where(lane_iota == K + j, lower1[j], top)
    tri_out[pl.ds(0, K), :] = top[:, : 2 * K]
    exchange_finish(1, zb)
    for b in range(M):
        wb[b] = apply(inverse, zb, b) - wb[b]
    tile = gram(wb, q2, 0, zero)
    tile = gram(wb, wb, K, tile)
    reduce_start(1, tile)

    total = reduce_finish(1)
    at_cols = columns(total, 0)
    s_cols = columns(total, K)
    a2_cols = rows_of(total)
    ata = matmul_cols(at_cols, a2_cols)
    for b in range(M):
        wb[b] = wb[b] - apply(at_cols, q2, b)
    order_root = math.sqrt(NR * NC * M * LANES)
    inverse, _, _ = factor([s - t for s, t in zip(s_cols, ata)])
    inverse = [v * order_root for v in inverse]
    for b in range(M):
        next_out[:, pl.ds(LANES * b, LANES)] = apply(inverse, wb, b)
    low = zero
    for j in range(K):
        low = jnp.where(lane_iota == j, upper1[j], low)
        low = jnp.where(lane_iota == K + j, a2_cols[j], low)
    tri_out[pl.ds(K, K), :] = low[:, : 2 * K]

    sent = 2 * (2 * (NC - 1) + NR - 1)
    wait_bytes(bl.at[pl.ds(0, sent // 2)], send_sem.at[0])
    wait_bytes(res_d.at[pl.ds(0, sent + 2 * (NR * NC - 1))], send_sem.at[1])
    wait_bytes(ar.at[0, pl.ds(0, NR + NC - 2)], send_sem.at[2])


def write_out(block, projection, block_out, projection_out, sems):
    copies = [
        pltpu.make_async_copy(block, block_out, sems.at[0]),
        pltpu.make_async_copy(projection, projection_out, sems.at[1]),
    ]
    for copy in copies:
        copy.start()
    for copy in copies:
        copy.wait()


def per_device(start_block, blocks, block_rows, block_cols, counts):
    args = (start_block, blocks, block_rows, block_cols, counts.T)
    vmem = pl.BlockSpec(memory_space=pltpu.VMEM)
    hbm = pl.BlockSpec(memory_space=pltpu.HBM)
    tile = (K, LANES)
    pair = (2 * K, LANES)
    block, projection = pl.pallas_call(
        kernel,
        out_shape=(
            jax.ShapeDtypeStruct((K, M * LANES), F32),
            jax.ShapeDtypeStruct((2 * K, 2 * K), F32),
        ),
        in_specs=[hbm] * 5,
        out_specs=(vmem, vmem),
        scratch_shapes=[
            pltpu.VMEM((SLOTS, LANES, LANES), BF16),
            pltpu.VMEM((SLOTS, LANES, LANES), BF16),
            pltpu.VMEM((K, M * LANES), F32),
            pltpu.SMEM((2, 1, SLOTS), jnp.int32),
            pltpu.SMEM((NC, NR), jnp.int32),
            pltpu.VMEM((2, 1, SLOTS), jnp.int32),
            *[pltpu.VMEM((M, *tile), F32)] * 7,
            pltpu.VMEM((2, M // 2, *pair), I16),
            pltpu.VMEM((2, 1, LANES), F32),
            pltpu.VMEM((2, NC, M // 2, *pair), I16),
            pltpu.VMEM((2, NC, 1, LANES), F32),
            pltpu.VMEM((2, NR, M // 2, *pair), I16),
            pltpu.VMEM((2, NR, 1, LANES), F32),
            pltpu.VMEM((NC + NR, *tile), F32),
            pltpu.VMEM((RB, *pair), BF16),
            pltpu.VMEM((CB, *pair), BF16),
            pltpu.VMEM((RB, 2 * SLOTS), BF16),
            pltpu.VMEM((CB, 2 * SLOTS), BF16),
            pltpu.VMEM((2, *tile), F32),
            pltpu.VMEM(((K + 1) * PITCH, LANES), F32),
            pltpu.VMEM(((K + 1) * PITCH, LANES), F32),
            pltpu.VMEM((2, NC, K // 2, *pair), I16),
            pltpu.VMEM((2, NR, K // 2, *pair), I16),
            pltpu.VMEM((2, 1, LANES), F32),
            pltpu.VMEM((2, 1, LANES), F32),
            pltpu.VMEM((2, NC, K // 2, *pair), I16),
            pltpu.VMEM((2, NR, K // 2, *pair), I16),
            pltpu.VMEM((2, NC, 1, LANES), F32),
            pltpu.VMEM((2, NR, 1, LANES), F32),
            pltpu.VMEM(((K + 1) * M, LANES), F32),
            pltpu.VMEM((2, 1, LANES), F32),
            pltpu.VMEM((2, NR * NC, 1, LANES), F32),
            pltpu.VMEM((2, 1, LANES), F32),
            pltpu.VMEM((NR, 1, LANES), F32),
            pltpu.VMEM((NC, 1, LANES), F32),
            pltpu.SemaphoreType.DMA((5,)),
            pltpu.SemaphoreType.DMA((20,)),
            pltpu.SemaphoreType.DMA((20,)),
        ],
        compiler_params=pltpu.CompilerParams(
            collective_id=0,
            has_side_effects=True,
            vmem_limit_bytes=48 * 1024 * 1024,
        ),
        name="lanczos",
    )(*[pltpu.with_memory_space_constraint(v, pltpu.HBM) for v in args])
    return pl.pallas_call(
        write_out,
        out_shape=(
            jax.ShapeDtypeStruct(block.shape, F32),
            jax.ShapeDtypeStruct(projection.shape, F32),
        ),
        in_specs=[vmem, vmem],
        out_specs=(hbm, hbm),
        scratch_shapes=[pltpu.SemaphoreType.DMA((2,))],
        name="write_out",
    )(
        pltpu.with_memory_space_constraint(block, pltpu.VMEM),
        pltpu.with_memory_space_constraint(projection, pltpu.VMEM),
    )


def solution(mesh):
    assert mesh.shape["row"] == NR and mesh.shape["col"] == NC
    both = ("row", "col")
    return jax.shard_map(
        per_device,
        mesh=mesh,
        in_specs=(
            P(None, both),
            P("row", "col", None, None, None),
            P(None, "col", None),
            P(None, "col", None),
            P(),
        ),
        out_specs=(P(None, both), P()),
        check_vma=False,
    )
```
